128 devices in a mesh: tm: 32 (over y, x, core), panel: 4 (over z).
Axes of the slice: x: 4, y: 4, z: 4, core: 2. Of those that a mesh axis runs over, the one named last changes fastest.
Arguments:
- observed: bfloat16 [16384, 4096], P('tm', 'panel'), may hold values from -12 to 12
- present: int32 [128, 4096], P('tm', 'panel'), may hold values 0 or 1
- loadings: bfloat16 [4096, 256], P('panel'), may hold values from -0.09375 to 0.09375
- noise_var: float32 [4096], P('panel'), may hold values from 1 to 4
- decay_rate: float32 [256], replicated, may hold values from 6.1035157e-06 to 0.03
- panel_of_block: int32 [32], P('panel'), may hold values from 0 to 18
Outputs:
- smoothed: float32 [16384, 256], P('tm')
- loading_moment: float32 [256, 4096], P('tm', 'panel')
- state_moment: float32 [256, 256], replicated
- panel_var: float32 [19], replicated
The draws below stay inside these ranges and needn't reach their ends.
All inputs are finite; a program needn't handle non-finite values. No bound on the sum of `present` on one device may be relied on, other than what follows from the above.
Results may differ from the reference program's by a relative error of at most 0.00055.
Values sent between devices are 32-bit elements; how exact they have to be, the bound alone decides.
No kernel may reach another device: no remote copies, remote signals or barrier semaphores. Data moves between devices by JAX's collectives and lax.ppermute only.
A program may use at most 128 MiB of HBM per device.

```python
import math
import jax
import jax.numpy as jnp
from jax import lax

S = 256
P_SIZE = 4096
SER_BLOCK = 128
PANELS = 19
BLOCK = 128
TIME = 16384
NB_ALL = 128


def loading_table(key):
    key_pick, key_scale, key_values = jax.random.split(key, 3)
    order = jax.random.permutation(key_pick, S)
    strong = order < S // 2
    spread = jax.random.uniform(key_scale, (S,), jnp.float32, 0.0, 1.0)
    column_scale = jnp.where(strong, 0.25 * 4.0 ** spread, 0.004 * 4.0 ** spread)
    values = jax.random.truncated_normal(key_values, -5.9, 5.9, (P_SIZE, S), jnp.float32)
    return values * column_scale[None, :] * P_SIZE ** (-0.5)


def draw_loadings(key, part):
    return loading_table(jax.random.fold_in(key, 101)).astype(jnp.bfloat16)


def draw_observed(key, part):
    loads = loading_table(jax.random.fold_in(key, 101)).astype(jnp.bfloat16).astype(jnp.float32)
    key_rate, key_start, key_steps, key_noise = jax.random.split(jax.random.fold_in(key, 202), 4)
    rate = 0.002 * 10.0 ** jax.random.uniform(key_rate, (S,), jnp.float32, 0.0, 1.0)
    amplitude = 4.0
    keep = 1.0 - rate
    kick = amplitude * jnp.sqrt(1.0 - keep * keep)
    start = amplitude * jax.random.normal(key_start, (S,), jnp.float32)
    shocks = jax.random.normal(key_steps, (TIME, S), jnp.float32)

    def advance(state, shock_row):
        following = keep * state + kick * shock_row
        return (following, following)
    unused_state, factors = lax.scan(advance, start, shocks)
    noise = jax.random.truncated_normal(key_noise, -6.0, 6.0, (TIME, P_SIZE), jnp.float32)
    signal = jnp.dot(factors, loads.T, precision=lax.Precision.HIGHEST)
    return jnp.clip(signal + noise, -12.0, 12.0).astype(jnp.bfloat16)


def place_ends(drawn, key, smallest, largest):
    longest = drawn.shape.index(max(drawn.shape))
    spots = []
    for shift in (0, 1):
        where = [jax.random.randint(jax.random.fold_in(key, axis), (), 0, length) for axis, length in enumerate(drawn.shape)]
        where[longest] = (where[longest] + shift) % drawn.shape[longest]
        spots.append(tuple(where))
    return drawn.at[spots[0]].set(smallest).at[spots[1]].set(largest)


def block_scale(stream_key, shape, pieces, least, high):
    gain = 1.0
    for dim, shards_of in pieces:
        draws = jax.random.uniform(jax.random.fold_in(jax.random.fold_in(stream_key, 6), dim), (shards_of,), jnp.float32, least / len(pieces), high / len(pieces))
        gain = gain * jnp.repeat(jnp.exp(draws), shape[dim] // shards_of).reshape((-1,) + (1,) * (len(shape) - 1 - dim))
    return gain


def setup_inputs(seed: int = 0) -> dict:
    key_of = jax.random.split(jax.random.key(seed), 7)
    observed = draw_observed(jax.random.fold_in(key_of[6], 71), 0)
    present = place_ends((jax.random.randint(key_of[1], (NB_ALL, P_SIZE), 0, 4) < 3).astype(jnp.int32), jax.random.fold_in(key_of[1], 1), 0, 1)
    loadings = draw_loadings(jax.random.fold_in(key_of[6], 71), 0)
    noise_var = jnp.clip(jnp.exp(math.log(4.0) - 1.3862944 * jax.random.uniform(key_of[3], (P_SIZE,), jnp.float32) ** block_scale(key_of[3], (P_SIZE,), ((0, 4),), -0.2, 0.2)), 1.0, 4.0)
    decay_rate = jnp.clip(jnp.exp(jax.random.uniform(key_of[4], (S,), jnp.float32, math.log(6.10351571594947e-06), math.log(0.03))), 6.10351571594947e-06, 0.03)
    panel_of_block = place_ends(jax.random.randint(key_of[5], (P_SIZE // SER_BLOCK,), 0, PANELS), jax.random.fold_in(key_of[5], 1), 0, PANELS - 1).astype(jnp.int32)
    return {"observed": observed, "present": present, "loadings": loadings, "noise_var": noise_var, "decay_rate": decay_rate, "panel_of_block": panel_of_block}


HIGH = lax.Precision.HIGHEST

def invert_one(gram_block):
    identity = jnp.eye(S, dtype=jnp.float32)
    factor = jnp.linalg.cholesky(identity + gram_block)
    return jax.scipy.linalg.cho_solve((factor, True), identity)

def reference(observed, present, loadings, noise_var, decay_rate, panel_of_block):
    loads = loadings.astype(jnp.float32)
    inv_noise = 1.0 / noise_var
    kept_mask = present.astype(jnp.float32)
    weighted = loads * inv_noise[:, None]

    def gram_one(mask_row):
        return jnp.dot((weighted * mask_row[:, None]).T, loads, precision=HIGH)
    gram_sum = lax.map(gram_one, kept_mask)
    inverse = lax.map(invert_one, gram_sum)
    persist = 1.0 - decay_rate
    transit = inverse * persist[None, None, :]
    obs_kept = observed.astype(jnp.float32).reshape(NB_ALL, BLOCK, P_SIZE) * kept_mask[:, None, :]
    projected = jnp.dot((obs_kept * inv_noise).reshape(TIME, P_SIZE), loads, precision=HIGH)
    inputs = jnp.einsum('bts,brs->btr', projected.reshape(NB_ALL, BLOCK, S), inverse, precision=HIGH)

    def run_block(state, block_pair):
        matrix, block_rows = block_pair

        def advance(carried, input_row):
            following = jnp.dot(matrix, carried, precision=HIGH) + input_row
            return (following, following)
        return lax.scan(advance, state, block_rows, reverse=False)

    def run_block_back(state, block_pair):
        matrix, block_rows = block_pair

        def advance(carried, input_row):
            following = jnp.dot(matrix, carried, precision=HIGH) + input_row
            return (following, following)
        return lax.scan(advance, state, block_rows, reverse=True)
    start_state = jnp.zeros((S,), jnp.float32)
    final_state, filtered = lax.scan(run_block, start_state, (transit, inputs))
    offsets = filtered - jnp.einsum('btr,bsr->bts', filtered * persist, transit, precision=HIGH)
    offsets = offsets.at[-1, -1].set(filtered[-1, -1])
    first_state, smooth_rows = lax.scan(run_block_back, start_state, (transit, offsets), reverse=True)
    smoothed = smooth_rows.reshape(TIME, S)
    state_moment = jnp.dot(smoothed.T, smoothed, precision=HIGH) / TIME
    flat_kept = obs_kept.reshape(TIME, P_SIZE)
    loading_moment = jnp.dot(smoothed.T, flat_kept, precision=HIGH) / math.sqrt(TIME)
    fitted = jnp.dot(smoothed, loads.T, precision=HIGH).reshape(NB_ALL, BLOCK, P_SIZE) * kept_mask[:, None, :]
    errors = obs_kept - fitted
    square_sums = lax.optimization_barrier(jnp.sum(errors * errors, axis=(0, 1)))
    obs_counts = BLOCK * lax.optimization_barrier(jnp.sum(kept_mask, axis=0))
    onehot = (panel_of_block[:, None] == jnp.arange(PANELS, dtype=jnp.int32)[None, :]).astype(jnp.float32)
    panel_sums = jnp.dot(square_sums.reshape(-1, SER_BLOCK).sum(axis=1), onehot, precision=HIGH)
    panel_counts = jnp.dot(obs_counts.reshape(-1, SER_BLOCK).sum(axis=1), onehot, precision=HIGH)
    panel_var = panel_sums / jnp.maximum(panel_counts, 1.0)
    return (smoothed, loading_moment, state_moment, panel_var)
```

```python
import functools
import math

import jax
import jax.numpy as jnp
from jax import lax
from jax.experimental import pallas as pl
from jax.experimental.pallas import tpu as pltpu
from jax.sharding import Mesh
from jax.sharding import PartitionSpec as P

SER_BLOCK = 128
PANELS = 19
LEVELS = 7
BLOCK = 128
TM = ("tm_0", "tm_1", "tm_2")
F32 = jnp.float32
BF16 = jnp.bfloat16
HIGH = lax.Precision.HIGHEST
VMEM = pl.BlockSpec(memory_space=pltpu.VMEM)
SMEM = pl.BlockSpec(memory_space=pltpu.SMEM)


def split(x):
    hi = x.astype(BF16)
    return hi, (x - hi.astype(F32)).astype(BF16)


def dot(a, b, dims=((1,), (0,))):
    return lax.dot_general(a, b, (dims, ((), ())), preferred_element_type=F32)


def dot3(a, b, dims=((1,), (0,))):
    return dot(a[0], b[0], dims) + (dot(a[0], b[1], dims) + dot(a[1], b[0], dims))


def grid_iota(n, axis):
    return lax.broadcasted_iota(jnp.int32, (n, n), axis)


def eye(n):
    return (grid_iota(n, 0) == grid_iota(n, 1)).astype(F32)


def pack(sym):
    n = sym.shape[0] // 2
    first, corner, second = sym[:n, :n], sym[:n, n:], sym[n:, n:]
    mixed = jnp.where(grid_iota(n, 0) >= grid_iota(n, 1), first, second)
    diag = jnp.sum(second * eye(n), axis=0, keepdims=True)
    return corner, mixed, jnp.broadcast_to(diag, (8, n))


def store_packed(ref, sym):
    n = sym.shape[0] // 2
    corner, mixed, diag = pack(sym)
    ref[0:n, :] = corner
    ref[n : 2 * n, :] = mixed
    ref[2 * n :, :] = diag


def unpack(packed):
    n = packed.shape[1]
    corner, mixed, diag = packed[:n], packed[n : 2 * n], packed[2 * n : 2 * n + 1]
    turned = mixed.T
    row, col = grid_iota(n, 0), grid_iota(n, 1)
    first = jnp.where(row >= col, mixed, turned)
    second = jnp.where(row == col, diag, jnp.where(row < col, mixed, turned))
    return jnp.concatenate(
        [jnp.concatenate([first, corner], axis=1), jnp.concatenate([corner.T, second], axis=1)],
        axis=0,
    )


def gram_kernel(place, present, noise, loads, *outs):
    coef = loads[...]
    turned = coef.astype(F32).T
    inv_noise = 1.0 / noise[...]
    for k in range(len(outs)):
        b = lax.rem(place[0] + k, len(outs))
        weight = present[pl.ds(b, 1), :].astype(F32) * inv_noise
        hi, lo = split(turned * weight)
        store_packed(outs[k], dot(hi, coef) + dot(lo, coef))


def project_kernel(place, present, noise, loads, observed, *outs):
    coef = loads[...]
    inv_noise = 1.0 / noise[...]
    for k in range(len(outs)):
        b = lax.rem(place[0] + k, len(outs))
        weight = present[pl.ds(b, 1), :].astype(F32) * inv_noise
        rows = observed[pl.ds(pl.multiple_of(b * BLOCK, BLOCK), BLOCK), :].astype(F32)
        hi, lo = split(rows * weight)
        outs[k][...] = dot(hi, coef) + dot(lo, coef)


def inverse_kernel(decay, g0, g1, g2, g3, out, guess):
    gram = unpack((g0[...] + g1[...]) + (g2[...] + g3[...]))
    n = gram.shape[0]
    ident = eye(n)
    whole = ident + gram
    size = jnp.max(jnp.sum(jnp.abs(gram), axis=1, keepdims=True))
    frob = jnp.sqrt(jnp.max(jnp.sum(jnp.sum(gram * gram, axis=1, keepdims=True), axis=0, keepdims=True)))
    top = 1.0 + jnp.minimum(size, frob) * 1.001
    scale = 2.0 / (1.0 + top)
    start = (top - 1.0) / (top + 1.0)
    guess[...] = (2.0 * scale) * ident - (scale * scale) * whole

    def improve(x):
        rest = 2.0 * ident - jnp.dot(whole, x, precision=HIGH, preferred_element_type=F32)
        return jnp.dot(x, rest, precision=HIGH, preferred_element_type=F32)

    def body(err):
        guess[...] = improve(guess[...])
        return err * err

    lax.while_loop(lambda err: err > 1e-4, body, start * start)
    inverse = improve(guess[...])
    gain = jnp.dot(gram, inverse, precision=HIGH, preferred_element_type=F32)
    gain = 0.5 * (gain + gain.T)
    rho = 1.0 - decay[...]
    root = jnp.sqrt(rho)
    root_down = jnp.sum(ident * root, axis=1, keepdims=True)
    store_packed(out, ident * (1.0 - rho) + gain * root * root_down)


def shifted(rows, offset, ahead):
    n = rows.shape[0]
    at = lax.broadcasted_iota(jnp.int32, rows.shape, 0)
    if ahead:
        return jnp.where(at >= offset, pltpu.roll(rows, offset, 0), 0.0)
    return jnp.where(at < n - offset, pltpu.roll(rows, n - offset, 0), 0.0)


def powers_kernel(place, decay, p0, p1, p2, p3, e0, e1, e2, e3, rows, his, los, tops, whole, errs, values):
    nb = 4
    root_inv = lax.rsqrt(1.0 - decay[...])
    for k, (p, e) in enumerate(((p0, e0), (p1, e1), (p2, e2), (p3, e3))):
        b = lax.rem(place[0] + nb - k, nb)
        errs[b] = unpack(e[...])
        values[b] = p[...] * root_inv
    for b in range(nb):
        err = errs[b]
        pair = split(err)
        z = values[b]
        y = z - dot3(split(z), pair)
        values[b] = y
        rows[b] = y
    for level in range(LEVELS):
        for b in range(nb):
            err = errs[b]
            pair = split(err)
            his[level * nb + b] = pair[0]
            los[level * nb + b] = pair[1]
            v = values[b]
            values[b] = v + shifted(v - dot3(split(v), pair), 1 << level, True)
            errs[b] = 2.0 * err - dot3(pair, pair)
    total, end = errs[0], values[0][BLOCK - 8 :]
    tops[0] = total
    for b in range(1, nb):
        err = errs[b]
        tops[b] = err
        pair = split(err)
        end = end - dot3(split(end), pair) + values[b][BLOCK - 8 :]
        total = total + err - dot3(split(total), pair)
    n = total.shape[0]
    whole[0:n, :] = total
    whole[n:, :] = jnp.broadcast_to(end[7:8], end.shape)


def join(maps):
    n = maps[0].shape[1]
    total, end = maps[0][:n], maps[0][n:]
    for m in maps[1:]:
        err = m[:n]
        pair = split(err)
        end = end - dot3(split(end), pair) + m[n:]
        total = total + err - dot3(split(total), pair)
    return total, end


def pair_kernel(place, mine, other, out):
    n = mine.shape[1]
    own, far = mine[...], other[...]
    first = place[0] == 0
    total, end = join([jnp.where(first, own, far), jnp.where(first, far, own)])
    out[0:n, :] = total
    out[n:, :] = end


def ordered(place, refs, scratch):
    for k, r in enumerate(refs):
        scratch[lax.rem(place + len(refs) - k, len(refs))] = r[...]


def group_kernel(place, m0, m1, m2, m3, out, scratch):
    n = m0.shape[1]
    ordered(place[0], (m0, m1, m2, m3), scratch)
    total, end = join([scratch[k] for k in range(4)])
    out[0:n, :] = total
    out[n:, :] = end


def advance(state, m):
    n = state.shape[1]
    return state - dot3(split(state), split(m[:n])) + m[n:]


def retreat(state, err):
    return state - dot3(split(state), split(err), ((1,), (1,)))


def scan_rows(values, his, los, nb, ahead):
    for level in range(LEVELS):
        for b in range(nb):
            v = values[b]
            pair = (his[level * nb + b], los[level * nb + b])
            values[b] = v + shifted(v - dot3(split(v), pair), 1 << level, ahead)


def forward_kernel(place, decay, y0, y1, y2, y3, x0, x1, x2, x3, mine, other, rows, his, los, tops,
                   past, change, first, ys, xs, values, states, states_b):
    nb = 4
    ordered(place[0], (y0, y1, y2, y3), ys)
    ordered(place[1], (x0, x1, x2, x3), xs)
    n = decay.shape[1]
    state = jnp.zeros((8, n), F32)
    state = lax.fori_loop(0, place[0], lambda k, s: advance(s, ys[k]), state)
    state = lax.fori_loop(0, place[1], lambda k, s: advance(s, xs[k]), state)
    state = jnp.where(place[2] == 0, state, advance(state, other[...]))
    at = lax.broadcasted_iota(jnp.int32, (BLOCK, n), 0)
    rho = 1.0 - decay[...]

    for b in range(nb):
        values[b] = rows[b]
    scan_rows(values, his, los, nb, True)
    for b in range(nb):
        states[b] = state
        state = state - dot3(split(state), split(tops[b])) + values[b][BLOCK - 1 :]
    for b in range(nb):
        s = states[b]
        pair = (his[b], los[b])
        step = s - dot3(split(s), pair)
        values[b] = rows[b] + jnp.where(at == 0, step[0:1], 0.0)
    scan_rows(values, his, los, nb, True)
    for b in range(nb):
        v = values[b]
        before = jnp.where(at == 0, states[b][0:1], pltpu.roll(v, 1, 0)) * rho
        past[b] = before
        change[b] = v - before
        values[b] = v - before
    scan_rows(values, his, los, nb, False)
    back = jnp.zeros((8, n), F32)
    for b in reversed(range(nb)):
        back = back - dot3(split(back), split(tops[b])) + values[b][0:1]
    first[...] = back


def pair_back_kernel(place, own, far, mine, other, out):
    n = mine.shape[1]
    lead = place[0] == 0
    early_q = jnp.where(lead, own[...], far[...])
    late_q = jnp.where(lead, far[...], own[...])
    early = jnp.where(lead, mine[0:n, :], other[0:n, :])
    out[...] = early_q + retreat(late_q, early)


def group_back_kernel(place, q0, q1, q2, q3, x0, x1, x2, x3, out, qs, xs):
    n = x0.shape[1]
    ordered(place[0], (q0, q1, q2, q3), qs)
    ordered(place[0], (x0, x1, x2, x3), xs)
    q = qs[3]
    for k in (2, 1, 0):
        q = qs[k] + retreat(q, xs[k][:n])
    out[...] = q


def final_kernel(place, panel_of, decay, gy0, gy1, gy2, gy3, gx0, gx1, gx2, gx3, far,
                 y0, y1, y2, y3, x0, x1, x2, x3, other, past, change, his, los, tops,
                 observed, present, loads,
                 smoothed, own_part, far_part, small,
                 gys, gxs, ys, xs, values, states, moment):
    nb = 4
    ordered(place[0], (gy0, gy1, gy2, gy3), gys)
    ordered(place[1], (gx0, gx1, gx2, gx3), gxs)
    ordered(place[0], (y0, y1, y2, y3), ys)
    ordered(place[1], (x0, x1, x2, x3), xs)
    n = decay.shape[1]
    nseg = 4
    back = jnp.zeros((8, n), F32)

    def over(gs, ms):
        def step(k, s):
            j = nseg - 1 - k
            return gs[j] + retreat(s, ms[j][:n])
        return step

    back = lax.fori_loop(0, nseg - 1 - place[0], over(gys, ys), back)
    back = lax.fori_loop(0, nseg - 1 - place[1], over(gxs, xs), back)
    back = jnp.where(place[2] == 0, far[...] + retreat(back, other[0:n, :]), back)
    at = lax.broadcasted_iota(jnp.int32, (BLOCK, n), 0)
    for b in range(nb):
        values[b] = change[b]
    scan_rows(values, his, los, nb, False)
    for b in reversed(range(nb)):
        states[b] = back
        back = back - dot3(split(back), split(tops[b])) + values[b][0:1]
    for b in range(nb):
        s = states[b]
        step = s - dot3(split(s), (his[b], los[b]))
        values[b] = change[b] + jnp.where(at == BLOCK - 1, step[0:1], 0.0)
    scan_rows(values, his, los, nb, False)
    root_inv = lax.rsqrt(1.0 - decay[...])
    for b in range(nb):
        smoothed[b * BLOCK : (b + 1) * BLOCK, :] = (values[b] + past[b]) * root_inv
    rows = smoothed[...]
    pair = split(rows)
    coef = loads[...]
    series = coef.shape[0]
    total = 128 * BLOCK
    weight = present[...].astype(F32)
    kept = jnp.concatenate(
        [observed[b * BLOCK : (b + 1) * BLOCK, :].astype(F32) * weight[b : b + 1] for b in range(nb)],
        axis=0,
    )
    kept_low = kept.astype(BF16)
    both = ((0,), (0,))
    moment[...] = (dot(pair[0], kept_low, both) + dot(pair[1], kept_low, both)) * (1.0 / math.sqrt(total))
    for i in range(16):
        own_part[i] = moment[pl.ds(pl.multiple_of((2 * i + place[2]) * 8, 8), 8), :]
        far_part[i] = moment[pl.ds(pl.multiple_of((2 * i + 1 - place[2]) * 8, 8), 8), :]
    moment[:, 0:n] = dot3(pair, pair, both) * (1.0 / total)
    small[0:64, :] = moment[pl.ds(pl.multiple_of(place[3] * 64, 64), 64), 0:n]
    across = ((1,), (1,))
    fitted = dot(pair[0], coef, across) + dot(pair[1], coef, across)
    squares = jnp.zeros((1, series), F32)
    for b in range(nb):
        part = slice(b * BLOCK, (b + 1) * BLOCK)
        miss = kept[part] - fitted[part] * weight[b : b + 1]
        squares = squares + jnp.sum(miss * miss, axis=0, keepdims=True)
    counts = float(BLOCK) * jnp.sum(weight, axis=0, keepdims=True)
    lane = lax.broadcasted_iota(jnp.int32, (8, n), 1)
    line = lax.broadcasted_iota(jnp.int32, (8, n), 0)
    sums = jnp.zeros((8, n), F32)
    for j in range(series // SER_BLOCK):
        part = slice(j * SER_BLOCK, (j + 1) * SER_BLOCK)
        sq = jnp.sum(squares[:, part], axis=1, keepdims=True)
        ct = jnp.sum(counts[:, part], axis=1, keepdims=True)
        here = lane == panel_of[j]
        sums = sums + jnp.where(here & (line == 0), sq, 0.0) + jnp.where(here & (line == 1), ct, 0.0)
    small[64:72, :] = sums


def finish_kernel(place, s0, s1, s2, s3, out, var):
    sums = jnp.zeros((8, s0.shape[1]), F32)
    for k, s in enumerate((s0, s1, s2, s3)):
        at = lax.rem(place[0] + 4 - k, 4)
        out[pl.ds(pl.multiple_of(at * 64, 64), 64), :] = s[0:64, :]
        sums = sums + s[64:72, :]
    var[...] = jnp.broadcast_to(sums[0:1] / jnp.maximum(sums[1:2], 1.0), var.shape)


def call(kernel, outs, scratch, *args, smem=1, name=None, mib=40):
    shapes = [jax.ShapeDtypeStruct(s, d) for s, d in outs]
    specs = [SMEM] * smem + [VMEM] * (len(args) - smem)
    return pl.pallas_call(
        kernel,
        out_shape=shapes,
        in_specs=specs,
        out_specs=[VMEM] * len(outs),
        scratch_shapes=[pltpu.VMEM(s, d) for s, d in scratch],
        compiler_params=pltpu.CompilerParams(vmem_limit_bytes=mib << 20),
        name=name or kernel.__name__,
    )(*args)


def from_peers(arrays, axis):
    n = lax.axis_size(axis)
    out = [arrays[0]]
    for k in range(1, n):
        out.append(lax.ppermute(arrays[k], axis, [(i, (i + k) % n) for i in range(n)]))
    return out


def gather(array, axis):
    return from_peers([array] * lax.axis_size(axis), axis)


def swap(array, axis):
    return lax.ppermute(array, axis, [(0, 1), (1, 0)])


def per_device(observed, present, loadings, noise_var, decay_rate, panel_of_block):
    time_rows, series = observed.shape
    width = loadings.shape[1]
    nb = time_rows // BLOCK
    half = width // 2
    ay, ax, ac = TM
    iy, ix, ic, iz = (lax.axis_index(a) for a in (ay, ax, ac, "panel"))
    scalar = lambda *v: jnp.stack([jnp.int32(i) for i in v])
    at_z, at_x, at_c = scalar(iz), scalar(ix), scalar(ic)
    at_all = scalar(iy, ix, ic, iz)
    noise = noise_var.reshape(1, series)
    decay = decay_rate.reshape(1, width)
    packed = ((width + 8, half), F32)
    map_shape = ((width + 8, width), F32)
    vec = ((8, width), F32)

    grams = call(gram_kernel, [packed] * nb, [], at_z, present, noise, loadings)
    projs = call(project_kernel, [((BLOCK, width), F32)] * nb, [], at_z, present, noise, loadings, observed)
    grams = from_peers(grams, "panel")
    grams, projs = lax.optimization_barrier((grams, projs))
    projs = from_peers(projs, "panel")
    (err,) = call(inverse_kernel, [packed], [((width, width), F32)], decay, *grams, smem=0)
    proj = (projs[0] + projs[1]) + (projs[2] + projs[3])
    errs = gather(err, "panel")
    projs = gather(proj, "panel")
    rows3 = ((nb, BLOCK, width), F32)
    rows, his, los, tops, seg = call(
        powers_kernel,
        [rows3, ((LEVELS * nb, width, width), BF16), ((LEVELS * nb, width, width), BF16),
         ((nb, width, width), F32), map_shape],
        [((nb, width, width), F32), rows3],
        at_z, decay, *projs, *errs,
    )
    seg_far = swap(seg, ac)
    (pair,) = call(pair_kernel, [map_shape], [], at_c, seg, seg_far)
    pairs = gather(pair, ax)
    maps4 = ((4, width + 8, width), F32)
    (group,) = call(group_kernel, [map_shape], [maps4], at_x, *pairs)
    groups = gather(group, ay)
    vecs4 = ((4, 8, width), F32)
    past, change, first = call(
        forward_kernel,
        [rows3, rows3, vec],
        [maps4, maps4, rows3, vecs4, vecs4],
        at_all, decay, *groups, *pairs, seg, seg_far, rows, his, los, tops,
    )
    first_far = swap(first, ac)
    (pair_first,) = call(pair_back_kernel, [vec], [], at_c, first, first_far, seg, seg_far)
    pair_firsts = gather(pair_first, ax)
    (group_first,) = call(group_back_kernel, [vec], [vecs4, maps4], at_x, *pair_firsts, *pairs)
    group_firsts = gather(group_first, ay)
    part = ((16, 8, series), F32)
    smoothed, own_part, far_part, small = call(
        final_kernel,
        [((time_rows, width), F32), part, part, ((72, width), F32)],
        [vecs4, vecs4, maps4, maps4, rows3, vecs4, ((width, series), F32)],
        at_all, panel_of_block, decay, *group_firsts, *pair_firsts, first_far, *groups, *pairs,
        seg_far, past, change, his, los, tops, observed, present, loadings,
        smem=2, mib=56,
    )
    own_part = own_part + swap(far_part, ac)
    arrived = lax.all_to_all(own_part, (ay, ax), 0, 0, tiled=True)
    loading_moment = arrived.sum(axis=0)
    small = small + swap(small, ac)
    for axis in (ax, ay):
        s = gather(small, axis)
        small = (s[0] + s[1]) + (s[2] + s[3])
    state_moment, var = call(
        finish_kernel, [((width, width), F32), vec], [], at_z, *gather(small, "panel")
    )
    return smoothed, loading_moment, state_moment, var[0, :PANELS]


def solution(mesh):
    finer = Mesh(
        mesh.devices.reshape(4, 4, 2, mesh.shape["panel"]), ("tm_0", "tm_1", "tm_2", "panel")
    )
    in_specs = (P(TM, "panel"), P(TM, "panel"), P("panel", None), P("panel"), P(), P("panel"))
    out_specs = (P(TM, None), P(TM, "panel"), P(), P())
    return jax.shard_map(
        per_device, mesh=finer, in_specs=in_specs, out_specs=out_specs, check_vma=False
    )
```

```python
import math

import jax
import jax.numpy as jnp
from jax import lax
from jax.experimental import pallas as pl
from jax.experimental.pallas import tpu as pltpu
from jax.sharding import Mesh
from jax.sharding import PartitionSpec as P


SER_BLOCK = 128
PANELS = 19
LEVELS = 7
BLOCK = 128
TM = ("tm_0", "tm_1", "tm_2")
F32 = jnp.float32
BF16 = jnp.bfloat16
HIGH = lax.Precision.HIGHEST
VMEM = pl.BlockSpec(memory_space=pltpu.VMEM)
SMEM = pl.BlockSpec(memory_space=pltpu.SMEM)


def split(x):
    hi = x.astype(BF16)
    return hi, (x - hi.astype(F32)).astype(BF16)


def dot(a, b, dims=((1,), (0,))):
    return lax.dot_general(a, b, (dims, ((), ())), preferred_element_type=F32)


def dot3(a, b, dims=((1,), (0,))):
    return dot(a[0], b[0], dims) + (dot(a[0], b[1], dims) + dot(a[1], b[0], dims))


def grid_iota(n, axis):
    return lax.broadcasted_iota(jnp.int32, (n, n), axis)


def eye(n):
    return (grid_iota(n, 0) == grid_iota(n, 1)).astype(F32)


def pack(sym):
    n = sym.shape[0] // 2
    first, corner, second = sym[:n, :n], sym[:n, n:], sym[n:, n:]
    mixed = jnp.where(grid_iota(n, 0) >= grid_iota(n, 1), first, second)
    diag = jnp.sum(second * eye(n), axis=0, keepdims=True)
    return corner, mixed, jnp.broadcast_to(diag, (8, n))


def store_packed(ref, sym):
    n = sym.shape[0] // 2
    corner, mixed, diag = pack(sym)
    ref[0:n, :] = corner
    ref[n : 2 * n, :] = mixed
    ref[2 * n : 2 * n + 8, :] = diag


def unpack(packed):
    n = packed.shape[1]
    corner, mixed, diag = packed[:n], packed[n : 2 * n], packed[2 * n : 2 * n + 1]
    turned = mixed.T
    row, col = grid_iota(n, 0), grid_iota(n, 1)
    first = jnp.where(row >= col, mixed, turned)
    second = jnp.where(row == col, diag, jnp.where(row < col, mixed, turned))
    return jnp.concatenate(
        [jnp.concatenate([first, corner], axis=1), jnp.concatenate([corner.T, second], axis=1)],
        axis=0,
    )


def gram_kernel(place, present_in, noise_in, loads_in, decay_in, turned, decay, o0, o1, o2, o3,
                present, noise, loads, sems):
    copies = [
        pltpu.make_async_copy(present_in, present, sems.at[0]),
        pltpu.make_async_copy(noise_in, noise, sems.at[1]),
        pltpu.make_async_copy(loads_in, loads, sems.at[2]),
        pltpu.make_async_copy(decay_in, decay, sems.at[3]),
    ]
    for c in copies:
        c.start()
    for c in copies:
        c.wait()
    coef = loads[...]
    flipped = coef.astype(F32).T
    turned[...] = flipped.astype(BF16)
    inv_noise = 1.0 / noise[...]
    for k, out in enumerate((o0, o1, o2, o3)):
        b = lax.rem(place[3] + k, 4)
        weight = present[pl.ds(b, 1), :].astype(F32) * inv_noise
        hi, lo = split(flipped * weight)
        store_packed(out, dot(hi, coef) + dot(lo, coef))


def project_kernel(place, present, noise, loads, observed, *outs):
    coef = loads[...]
    inv_noise = 1.0 / noise[...]
    for k in range(len(outs)):
        b = lax.rem(place[3] + k, len(outs))
        weight = present[pl.ds(b, 1), :].astype(F32) * inv_noise
        rows = observed[pl.ds(pl.multiple_of(b * BLOCK, BLOCK), BLOCK), :].astype(F32)
        hi, lo = split(rows * weight)
        outs[k][...] = dot(hi, coef) + dot(lo, coef)


def inverse_kernel(decay, g0, g1, g2, g3, out, guess):
    gram = unpack((g0[...] + g1[...]) + (g2[...] + g3[...]))
    n = gram.shape[0]
    ident = eye(n)
    whole = ident + gram
    size = jnp.max(jnp.sum(jnp.abs(gram), axis=1, keepdims=True))
    frob = jnp.sqrt(jnp.max(jnp.sum(jnp.sum(gram * gram, axis=1, keepdims=True), axis=0, keepdims=True)))
    top = 1.0 + jnp.minimum(size, frob) * 1.001
    scale = 2.0 / (1.0 + top)
    start = (top - 1.0) / (top + 1.0)
    guess[...] = (2.0 * scale) * ident - (scale * scale) * whole

    def improve(x):
        rest = 2.0 * ident - jnp.dot(whole, x, precision=HIGH, preferred_element_type=F32)
        return jnp.dot(x, rest, precision=HIGH, preferred_element_type=F32)

    def body(err):
        guess[...] = improve(guess[...])
        return err * err

    lax.while_loop(lambda err: err > 1e-4, body, start * start)
    inverse = improve(guess[...])
    gain = jnp.dot(gram, inverse, precision=HIGH, preferred_element_type=F32)
    gain = 0.5 * (gain + gain.T)
    rho = 1.0 - decay[...]
    root = jnp.sqrt(rho)
    root_down = jnp.sum(ident * root, axis=1, keepdims=True)
    store_packed(out, ident * (1.0 - rho) + gain * root * root_down)


def shifted(rows, offset, ahead):
    n = rows.shape[0]
    at = lax.broadcasted_iota(jnp.int32, rows.shape, 0)
    if ahead:
        return jnp.where(at >= offset, pltpu.roll(rows, offset, 0), 0.0)
    return jnp.where(at < n - offset, pltpu.roll(rows, n - offset, 0), 0.0)


def end_kernel(decay, packed, p0, p1, p2, p3, total, out, err_ref):
    n = decay.shape[1]
    half = n // 2
    proj = (p0[...] + p1[...]) + (p2[...] + p3[...])
    total[...] = proj
    out[0 : n + 8, :] = packed[...]
    err = unpack(packed[...])
    z = proj * lax.rsqrt(1.0 - decay[...])
    v = z - dot3(split(z), split(err))
    err_ref[...] = err
    rows = BLOCK
    for level in range(LEVELS):
        pair = split(err_ref[...])
        v = v + shifted(v - dot3(split(v), pair), 1 << level, True)
        if level + 1 < LEVELS:
            err_ref[...] = 2.0 * err_ref[...] - dot3(pair, pair)
    out[n + 8 : n + 16, :] = jnp.broadcast_to(v[rows - 1 :, :half], (8, half))
    out[n + 16 :, :] = jnp.broadcast_to(v[rows - 1 :, half:], (8, half))


def powers_kernel(place, e0, e1, e2, e3, his, los, tops, ends, whole, errs):
    nb = 4
    n = 2 * e0.shape[1]
    half = n // 2
    for k, e in enumerate((e0, e1, e2, e3)):
        b = lax.rem(place[3] + nb - k, nb)
        errs[b] = unpack(e[0 : n + 8, :])
        ends[b, :, 0:half] = e[n + 8 : n + 16, :]
        ends[b, :, half:] = e[n + 16 :, :]
    for level in range(LEVELS):
        for b in range(nb):
            err = errs[b]
            pair = split(err)
            his[level * nb + b] = pair[0]
            los[level * nb + b] = pair[1]
            errs[b] = 2.0 * err - dot3(pair, pair)
    total, end = errs[0], ends[0]
    tops[0] = total
    for b in range(1, nb):
        err = errs[b]
        tops[b] = err
        pair = split(err)
        end = end - dot3(split(end), pair) + ends[b]
        total = total + err - dot3(split(total), pair)
    whole[0:n, :] = total
    whole[n:, :] = end


def join(maps):
    n = maps[0].shape[1]
    total, end = maps[0][:n], maps[0][n:]
    for m in maps[1:]:
        err = m[:n]
        pair = split(err)
        end = end - dot3(split(end), pair) + m[n:]
        total = total + err - dot3(split(total), pair)
    return total, end


def store_map(total, end, core, out, half):
    n = total.shape[1]
    h = n // 2
    out[0:n, :] = total
    out[n:, :] = end
    half[0:h, :] = out[pl.ds(pl.multiple_of(core * h, h), h), :]
    half[h:, :] = end


def pair_kernel(place, mine, other, out, half):
    own, far = mine[...], other[...]
    first = place[2] == 0
    total, end = join([jnp.where(first, own, far), jnp.where(first, far, own)])
    store_map(total, end, place[2], out, half)


def ordered(place, refs, scratch):
    for k, r in enumerate(refs):
        scratch[lax.rem(place + len(refs) - k, len(refs))] = r[...]


def ordered_maps(place, core, own, halves, maps):
    n = own.shape[1]
    h = n // 2
    maps[place] = own[...]
    for k, (mine, other) in enumerate(halves):
        at = lax.rem(place + 3 - k, 4)
        maps[at, pl.ds(pl.multiple_of(core * h, h), h), :] = mine[0:h, :]
        maps[at, pl.ds(pl.multiple_of((1 - core) * h, h), h), :] = other[0:h, :]
        maps[at, n:, :] = mine[h:, :]


def group_kernel(place, own, m1, m2, m3, o1, o2, o3, out, half, maps):
    ordered_maps(place[1], place[2], own, ((m1, o1), (m2, o2), (m3, o3)), maps)
    total, end = join([maps[k] for k in range(4)])
    store_map(total, end, place[2], out, half)


def advance(state, m):
    n = state.shape[1]
    return state - dot3(split(state), split(m[:n])) + m[n:]


def retreat(state, err):
    return state - dot3(split(state), split(err), ((1,), (1,)))


def scan_rows(values, his, los, nb, ahead):
    for level in range(LEVELS):
        for b in range(nb):
            v = values[b]
            pair = (his[level * nb + b], los[level * nb + b])
            values[b] = v + shifted(v - dot3(split(v), pair), 1 << level, ahead)


def forward_kernel(place, decay, own, m1, m2, m3, o1, o2, o3, xs, other, p0, p1, p2, p3,
                   ends, his, los, tops,
                   past, change, firsts, first, ys, values, states):
    nb = 4
    root_inv = lax.rsqrt(1.0 - decay[...])
    ordered(place[3], (p0, p1, p2, p3), values)
    ordered_maps(place[0], place[2], own, ((m1, o1), (m2, o2), (m3, o3)), ys)
    n = decay.shape[1]
    state = jnp.zeros((8, n), F32)
    state = lax.fori_loop(0, place[0], lambda k, s: advance(s, ys[k]), state)
    state = lax.fori_loop(0, place[1], lambda k, s: advance(s, xs[k]), state)
    state = jnp.where(place[2] == 0, state, advance(state, other[...]))
    at = lax.broadcasted_iota(jnp.int32, (BLOCK, n), 0)
    rho = 1.0 - decay[...]
    for b in range(nb):
        states[b] = state
        if b + 1 < nb:
            state = state - dot3(split(state), split(tops[b])) + ends[b]
    for b in range(nb):
        z = values[b] * root_inv
        z = z + jnp.where(at == 0, states[b][0:1], 0.0)
        values[b] = z - dot3(split(z), (his[b], los[b]))
    scan_rows(values, his, los, nb, True)
    for b in range(nb):
        v = values[b]
        before = jnp.where(at == 0, states[b][0:1], pltpu.roll(v, 1, 0)) * rho
        past[b] = before
        change[b] = v - before
        values[b] = v - before
    scan_rows(values, his, los, nb, False)
    back = jnp.zeros((8, n), F32)
    for b in reversed(range(nb)):
        lead = jnp.broadcast_to(values[b][0:1], (8, n))
        firsts[b] = lead
        back = back - dot3(split(back), split(tops[b])) + lead
    first[...] = back


def pair_back_kernel(place, own, far, mine, other, out):
    n = mine.shape[1]
    lead = place[2] == 0
    early_q = jnp.where(lead, own[...], far[...])
    late_q = jnp.where(lead, far[...], own[...])
    early = jnp.where(lead, mine[0:n, :], other[0:n, :])
    out[...] = early_q + retreat(late_q, early)


def group_back_kernel(place, q0, q1, q2, q3, xs, out, qs):
    n = xs.shape[2]
    ordered(place[1], (q0, q1, q2, q3), qs)
    q = qs[3]
    for k in (2, 1, 0):
        q = qs[k] + retreat(q, xs[k, 0:n, :])
    out[...] = q


def smooth_kernel(place, decay, gy0, gy1, gy2, gy3, gxs, far, ys, xs, other,
                  past, change, firsts, his, los, tops,
                  smoothed, high, low, quarter, gys, values, states, moment):
    nb = 4
    nseg = 4
    ordered(place[0], (gy0, gy1, gy2, gy3), gys)
    n = decay.shape[1]
    back = jnp.zeros((8, n), F32)

    def over(gs, ms):
        def step(k, s):
            j = nseg - 1 - k
            return gs[j] + retreat(s, ms[j, 0:n, :])

        return step

    back = lax.fori_loop(0, nseg - 1 - place[0], over(gys, ys), back)
    back = lax.fori_loop(0, nseg - 1 - place[1], over(gxs, xs), back)
    back = jnp.where(place[2] == 0, far[...] + retreat(back, other[0:n, :]), back)
    at = lax.broadcasted_iota(jnp.int32, (BLOCK, n), 0)
    for b in reversed(range(nb)):
        states[b] = back
        if b:
            back = back - dot3(split(back), split(tops[b])) + firsts[b]
    for b in range(nb):
        s = states[b]
        step = s - dot3(split(s), (his[b], los[b]))
        values[b] = change[b] + jnp.where(at == BLOCK - 1, step[0:1], 0.0)
    scan_rows(values, his, los, nb, False)
    root_inv = lax.rsqrt(1.0 - decay[...])
    for b in range(nb):
        smoothed[b * BLOCK : (b + 1) * BLOCK, :] = (values[b] + past[b]) * root_inv
    pair = split(smoothed[...])
    high[...], low[...] = pair
    moment[...] = dot3(pair, pair, ((0,), (0,))) * (1.0 / (128 * BLOCK))
    quarter[...] = moment[pl.ds(pl.multiple_of(place[3] * 64, 64), 64), :]


def errors_kernel(panel_of, high, low, observed, present, turned, sums_out):
    nb = 4
    n, series = turned.shape
    coef = turned[...]
    weight = present[...].astype(F32)
    squares = jnp.zeros((1, series), F32)
    for b in range(nb):
        part = slice(b * BLOCK, (b + 1) * BLOCK)
        miss = observed[part, :].astype(F32) - (dot(high[part, :], coef) + dot(low[part, :], coef))
        squares = squares + jnp.sum(miss * miss, axis=0, keepdims=True) * weight[b : b + 1]
    counts = float(BLOCK) * jnp.sum(weight, axis=0, keepdims=True)
    lane = lax.broadcasted_iota(jnp.int32, (8, n), 1)
    line = lax.broadcasted_iota(jnp.int32, (8, n), 0)
    sums = jnp.zeros((8, n), F32)
    for j in range(series // SER_BLOCK):
        part = slice(j * SER_BLOCK, (j + 1) * SER_BLOCK)
        sq = jnp.sum(squares[:, part], axis=1, keepdims=True)
        ct = jnp.sum(counts[:, part], axis=1, keepdims=True)
        here = lane == panel_of[j]
        sums = sums + jnp.where(here & (line == 0), sq, 0.0) + jnp.where(here & (line == 1), ct, 0.0)
    sums_out[...] = sums


def moment_kernel(place, high, low, observed, present, own_part, far_part, moment):
    nb = 4
    weight = present[...].astype(F32)
    kept = jnp.concatenate(
        [
            (observed[b * BLOCK : (b + 1) * BLOCK, :].astype(F32) * weight[b : b + 1]).astype(BF16)
            for b in range(nb)
        ],
        axis=0,
    )
    both = ((0,), (0,))
    scale = 1.0 / math.sqrt(128 * BLOCK)
    moment[...] = (dot(high[...], kept, both) + dot(low[...], kept, both)) * scale
    for i in range(16):
        own_part[i] = moment[pl.ds(pl.multiple_of((2 * i + place[2]) * 8, 8), 8), :]
        far_part[i] = moment[pl.ds(pl.multiple_of((2 * i + 1 - place[2]) * 8, 8), 8), :]


def add_kernel(a, b, out):
    out[...] = a[...] + b[...]


def small_kernel(q, q_far, s, s_far, out):
    out[0:64, :] = q[...] + q_far[...]
    out[64:72, :] = s[...] + s_far[...]


def sum_kernel(a, b, c, d, out):
    out[...] = (a[...] + b[...]) + (c[...] + d[...])


def finish_kernel(place, s0, s1, s2, s3, out, var):
    sums = jnp.zeros((8, s0.shape[1]), F32)
    for k, s in enumerate((s0, s1, s2, s3)):
        at = lax.rem(place[3] + 4 - k, 4)
        out[pl.ds(pl.multiple_of(at * 64, 64), 64), :] = s[0:64, :]
        sums = sums + s[64:72, :]
    var[...] = jnp.broadcast_to(sums[0:1] / jnp.maximum(sums[1:2], 1.0), var.shape)


def call(kernel, outs, scratch, *args, smem=1, far=0, sems=0, mib=12):
    shapes = [jax.ShapeDtypeStruct(s, d) for s, d in outs]
    specs = [SMEM] * smem + [pl.BlockSpec(memory_space=pltpu.HBM)] * far
    specs += [VMEM] * (len(args) - smem - far)
    made = pl.pallas_call(
        kernel,
        out_shape=shapes,
        in_specs=specs,
        out_specs=[VMEM] * len(outs),
        scratch_shapes=[pltpu.VMEM(s, d) for s, d in scratch]
        + ([pltpu.SemaphoreType.DMA((sems,))] if sems else []),
        compiler_params=pltpu.CompilerParams(vmem_limit_bytes=mib << 20),
    )
    return made(*args)


def from_peers(arrays, axis):
    n = lax.axis_size(axis)
    out = [arrays[0]]
    for k in range(1, n):
        out.append(lax.ppermute(arrays[k], axis, [(i, (i + k) % n) for i in range(n)]))
    return out


def gather(array, axis):
    return from_peers([array] * lax.axis_size(axis), axis)


def swap(array, axis):
    return lax.ppermute(array, axis, [(0, 1), (1, 0)])


def step(observed, present, loadings, noise_var, decay_rate, panel_of_block):
    time_rows, series = observed.shape
    width = loadings.shape[1]
    nb = time_rows // BLOCK
    half = width // 2
    ay, ax, ac = TM
    iy, ix, ic, iz = (lax.axis_index(a) for a in (ay, ax, ac, "panel"))
    scalar = lambda *v: jnp.stack([jnp.int32(i) for i in v])
    place = scalar(iy, ix, ic, iz)
    noise = noise_var.reshape(1, series)
    packed = ((width + 8, half), F32)
    packed_end = ((width + 24, half), F32)
    map_shape = ((width + 8, width), F32)
    half_shape = ((half + 8, width), F32)
    vec = ((8, width), F32)
    vecs4 = ((4, 8, width), F32)
    maps4 = ((4, width + 8, width), F32)
    rows2 = ((BLOCK, width), F32)
    rows3 = ((nb, BLOCK, width), F32)
    square = ((width, width), F32)
    squares4 = ((nb, width, width), F32)
    powers = ((LEVELS * nb, width, width), BF16)

    turned, decay, *grams = call(
        gram_kernel, [((width, series), BF16), ((1, width), F32)] + [packed] * nb,
        [(present.shape, jnp.int32), ((1, series), F32), ((series, width), BF16)],
        place, present, noise, loadings, decay_rate.reshape(1, width), far=4, sems=4,
    )
    projs = call(project_kernel, [rows2] * nb, [], place, present, noise, loadings, observed)
    grams = from_peers(grams, "panel")
    projs = from_peers(projs, "panel")
    (err,) = call(inverse_kernel, [packed], [square], decay, *grams, smem=0)
    proj, err_end = call(end_kernel, [rows2, packed_end], [square], decay, err, *projs, smem=0)
    errs = gather(err_end, "panel")
    his, los, tops, ends, seg = call(
        powers_kernel,
        [powers, powers, squares4, vecs4, map_shape],
        [squares4],
        place, *errs,
    )
    seg, proj = lax.optimization_barrier((seg, proj))
    seg_far = swap(seg, ac)
    projs = gather(proj, "panel")
    pair, pair_half = call(pair_kernel, [map_shape, half_shape], [], place, seg, seg_far)
    near = gather(pair_half, ax)[1:]
    group, group_half, xs = call(
        group_kernel, [map_shape, half_shape, maps4], [],
        place, pair, *near, *[swap(m, ac) for m in near],
    )
    near = gather(group_half, ay)[1:]
    past, change, firsts, first, ys = call(
        forward_kernel,
        [rows3, rows3, vecs4, vec, maps4],
        [rows3, vecs4],
        place, decay, group, *near, *[swap(m, ac) for m in near],
        xs, seg_far, *projs, ends, his, los, tops,
    )
    first_far = swap(first, ac)
    (pair_first,) = call(pair_back_kernel, [vec], [], place, first, first_far, seg, seg_far)
    group_first, gxs = call(
        group_back_kernel, [vec, vecs4], [], place, *gather(pair_first, ax), xs
    )
    flat = ((time_rows, width), BF16)
    smoothed, high, low, quarter = call(
        smooth_kernel,
        [((time_rows, width), F32), flat, flat, ((64, width), F32)],
        [vecs4, rows3, vecs4, square],
        place, decay, *gather(group_first, ay), gxs, first_far, ys, xs, seg_far,
        past, change, firsts, his, los, tops,
    )
    quarter_far = swap(quarter, ac)
    (sums,) = call(errors_kernel, [vec], [], panel_of_block, high, low, observed, present, turned)
    small_shape = ((72, width), F32)
    (small,) = call(small_kernel, [small_shape], [], quarter, quarter_far, sums, swap(sums, ac), smem=0)
    (small,) = call(sum_kernel, [small_shape], [], *gather(small, ax), smem=0)
    part = ((16, 8, series), F32)
    own_part, far_part = call(
        moment_kernel, [part, part], [((width, series), F32)], place, high, low, observed, present
    )
    (own_part,) = call(add_kernel, [part], [], own_part, swap(far_part, ac), smem=0)
    arrived = lax.all_to_all(own_part, (ay, ax), 0, 0, tiled=True)
    loading_moment = arrived.sum(axis=0)
    (small,) = call(sum_kernel, [small_shape], [], *gather(small, ay), smem=0)
    state_moment, var = call(finish_kernel, [square, vec], [], place, *gather(small, "panel"))
    return smoothed, loading_moment, state_moment, var[0, :PANELS]


def solution(mesh):
    finer = Mesh(
        mesh.devices.reshape(4, 4, 2, mesh.shape["panel"]), ("tm_0", "tm_1", "tm_2", "panel")
    )
    in_specs = (P(TM, "panel"), P(TM, "panel"), P("panel", None), P("panel"), P(), P("panel"))
    out_specs = (P(TM, None), P(TM, "panel"), P(), P())
    return jax.shard_map(step, mesh=finer, in_specs=in_specs, out_specs=out_specs, check_vma=False)
```

```python
import math

import jax
import jax.numpy as jnp
from jax import lax
from jax.experimental import pallas as pl
from jax.experimental.pallas import tpu as pltpu
from jax.sharding import Mesh
from jax.sharding import PartitionSpec as P


SER_BLOCK = 128
PANELS = 19
LEVELS = 7
BLOCK = 128
TM = ("tm_0", "tm_1", "tm_2")
F32 = jnp.float32
BF16 = jnp.bfloat16
HIGH = lax.Precision.HIGHEST
VMEM = pl.BlockSpec(memory_space=pltpu.VMEM)
SMEM = pl.BlockSpec(memory_space=pltpu.SMEM)


def split(x):
    hi = x.astype(BF16)
    return hi, (x - hi.astype(F32)).astype(BF16)


def dot(a, b, dims=((1,), (0,))):
    return lax.dot_general(a, b, (dims, ((), ())), preferred_element_type=F32)


def dot3(a, b, dims=((1,), (0,))):
    return dot(a[0], b[0], dims) + (dot(a[0], b[1], dims) + dot(a[1], b[0], dims))


def grid_iota(n, axis):
    return lax.broadcasted_iota(jnp.int32, (n, n), axis)


def eye(n):
    return (grid_iota(n, 0) == grid_iota(n, 1)).astype(F32)


def pack(sym):
    n = sym.shape[0] // 2
    first, corner, second = sym[:n, :n], sym[:n, n:], sym[n:, n:]
    mixed = jnp.where(grid_iota(n, 0) >= grid_iota(n, 1), first, second)
    diag = jnp.sum(second * eye(n), axis=0, keepdims=True)
    return corner, mixed, jnp.broadcast_to(diag, (8, n))


def store_packed(ref, sym):
    n = sym.shape[0] // 2
    corner, mixed, diag = pack(sym)
    ref[0:n, :] = corner
    ref[n : 2 * n, :] = mixed
    ref[2 * n : 2 * n + 8, :] = diag


def unpack(packed):
    n = packed.shape[1]
    corner, mixed, diag = packed[:n], packed[n : 2 * n], packed[2 * n : 2 * n + 1]
    turned = mixed.T
    row, col = grid_iota(n, 0), grid_iota(n, 1)
    first = jnp.where(row >= col, mixed, turned)
    second = jnp.where(row == col, diag, jnp.where(row < col, mixed, turned))
    return jnp.concatenate(
        [jnp.concatenate([first, corner], axis=1), jnp.concatenate([corner.T, second], axis=1)],
        axis=0,
    )


def gram_kernel(place, present, noise, loads, *outs):
    coef = loads[...]
    flipped = coef.astype(F32).T
    inv_noise = 1.0 / noise[...]
    for k, out in enumerate(outs):
        b = lax.rem(place[3] + k, len(outs))
        hi, lo = split(flipped * (present[pl.ds(b, 1), :].astype(F32) * inv_noise))
        store_packed(out, dot(hi, coef) + dot(lo, coef))


def project_kernel(place, present, noise, loads, decay, observed, table, *outs):
    coef = loads[...]
    inv_noise = 1.0 / noise[...]
    table[0:4, :] = present[...].astype(F32)
    table[4:5, 0 : decay.shape[1]] = decay[...]
    for k in range(len(outs)):
        b = lax.rem(place[3] + k, len(outs))
        rows = observed[pl.ds(pl.multiple_of(b * BLOCK, BLOCK), BLOCK), :].astype(F32)
        hi, lo = split(rows * (present[pl.ds(b, 1), :].astype(F32) * inv_noise))
        outs[k][...] = dot(hi, coef) + dot(lo, coef)


def turn_kernel(loads, out):
    out[...] = loads[...].astype(F32).T.astype(BF16)


def decay_of(table, n):
    return table[4:5, 0:n]


def inverse_kernel(table, g0, g1, g2, g3, out, guess):
    gram = unpack((g0[...] + g1[...]) + (g2[...] + g3[...]))
    n = gram.shape[0]
    ident = eye(n)
    whole = ident + gram
    size = jnp.max(jnp.sum(jnp.abs(gram), axis=1, keepdims=True))
    frob = jnp.sqrt(jnp.max(jnp.sum(jnp.sum(gram * gram, axis=1, keepdims=True), axis=0, keepdims=True)))
    top = 1.0 + jnp.minimum(size, frob) * 1.001
    scale = 2.0 / (1.0 + top)
    start = (top - 1.0) / (top + 1.0)
    guess[...] = (2.0 * scale) * ident - (scale * scale) * whole

    def improve(x):
        rest = 2.0 * ident - jnp.dot(whole, x, precision=HIGH, preferred_element_type=F32)
        return jnp.dot(x, rest, precision=HIGH, preferred_element_type=F32)

    def body(err):
        guess[...] = improve(guess[...])
        return err * err

    def quick(err):
        x = guess[...]
        pair = split(x)
        guess[...] = 2.0 * x - dot3(pair, split(dot3(split(whole), pair)))
        return err * err

    err = lax.while_loop(lambda e: (e > 1e-4) & (top < 8.0), quick, start * start)
    lax.while_loop(lambda e: e > 1e-4, body, err)
    inverse = improve(guess[...])
    gain = jnp.dot(gram, inverse, precision=HIGH, preferred_element_type=F32)
    gain = 0.5 * (gain + gain.T)
    rho = 1.0 - decay_of(table, n)
    root = jnp.sqrt(rho)
    root_down = jnp.sum(ident * root, axis=1, keepdims=True)
    store_packed(out, ident * (1.0 - rho) + gain * root * root_down)


def shifted(rows, offset, ahead):
    n = rows.shape[0]
    at = lax.broadcasted_iota(jnp.int32, rows.shape, 0)
    if ahead:
        return jnp.where(at >= offset, pltpu.roll(rows, offset, 0), 0.0)
    return jnp.where(at < n - offset, pltpu.roll(rows, n - offset, 0), 0.0)


def end_kernel(table, packed, p0, p1, p2, p3, total, out, err_ref):
    proj = (p0[...] + p1[...]) + (p2[...] + p3[...])
    total[...] = proj
    z = proj * lax.rsqrt(1.0 - decay_of(table, proj.shape[1]))
    err_ref[...] = unpack(packed[...])
    v = z - dot3(split(z), split(err_ref[...]))
    for level in range(LEVELS):
        pair = split(err_ref[...])
        v = v + shifted(v - dot3(split(v), pair), 1 << level, True)
        if level + 1 < LEVELS:
            err_ref[...] = 2.0 * err_ref[...] - dot3(pair, pair)
    out[...] = jnp.broadcast_to(v[BLOCK - 1 :], out.shape)


def powers_kernel(place, e0, e1, e2, e3, his, los, tops, whole, errs):
    nb = 4
    for k, e in enumerate((e0, e1, e2, e3)):
        errs[lax.rem(place[3] + nb - k, nb)] = unpack(e[...])

    def square(level, carry):
        for b in range(nb):
            err = errs[b]
            pair = split(err)
            his[level * nb + b] = pair[0]
            los[level * nb + b] = pair[1]
            errs[b] = 2.0 * err - dot3(pair, pair)
        return carry

    lax.fori_loop(0, LEVELS, square, 0)
    total = errs[0]
    tops[0] = total
    for b in range(1, nb):
        err = errs[b]
        tops[b] = err
        total = total + err - dot3(split(total), split(err))
    whole[...] = total


def segment_end_kernel(place, tops, v0, v1, v2, v3, ends, out):
    nb = 4
    ordered(place[3], (v0, v1, v2, v3), ends)
    end = ends[0]
    for b in range(1, nb):
        end = end - dot3(split(end), split(tops[b])) + ends[b]
    out[...] = end


def join(maps):
    n = maps[0].shape[1]
    total, end = maps[0][:n], maps[0][n:]
    for m in maps[1:]:
        err = m[:n]
        pair = split(err)
        end = end - dot3(split(end), pair) + m[n:]
        total = total + err - dot3(split(total), pair)
    return total, end


def store_map(total, end, core, out, half):
    n = total.shape[1]
    h = n // 2
    out[0:n, :] = total
    out[n:, :] = end
    half[0:h, :] = out[pl.ds(pl.multiple_of(core * h, h), h), :]
    half[h:, :] = end


def pair_kernel(place, mine, other, v_mine, v_other, out, half):
    own, far, v_own, v_far = mine[...], other[...], v_mine[...], v_other[...]
    first = place[2] == 0
    total = jnp.where(first, own, far)
    err = jnp.where(first, far, own)
    pair = split(err)
    end = jnp.where(first, v_own, v_far)
    end = end - dot3(split(end), pair) + jnp.where(first, v_far, v_own)
    total = total + err - dot3(split(total), pair)
    store_map(total, end, place[2], out, half)


def ordered(place, refs, scratch):
    for k, r in enumerate(refs):
        scratch[lax.rem(place + len(refs) - k, len(refs))] = r[...]


def ordered_maps(place, core, own, halves, maps):
    n = own.shape[1]
    h = n // 2
    maps[place] = own[...]
    for k, (mine, other) in enumerate(halves):
        at = lax.rem(place + 3 - k, 4)
        maps[at, pl.ds(pl.multiple_of(core * h, h), h), :] = mine[0:h, :]
        maps[at, pl.ds(pl.multiple_of((1 - core) * h, h), h), :] = other[0:h, :]
        maps[at, n:, :] = mine[h:, :]


def group_kernel(place, own, m1, m2, m3, o1, o2, o3, out, half, maps):
    ordered_maps(place[1], place[2], own, ((m1, o1), (m2, o2), (m3, o3)), maps)
    total, end = join([maps[k] for k in range(4)])
    store_map(total, end, place[2], out, half)


def advance(state, m):
    n = state.shape[1]
    return state - dot3(split(state), split(m[:n])) + m[n:]


def retreat(state, err):
    return state - dot3(split(state), split(err), ((1,), (1,)))


def scan_rows(values, his, los, nb, ahead):
    for level in range(LEVELS):
        for b in range(nb):
            v = values[b]
            pair = (his[level * nb + b], los[level * nb + b])
            values[b] = v + shifted(v - dot3(split(v), pair), 1 << level, ahead)


def forward_kernel(place, table, own, m1, m2, m3, o1, o2, o3, xs, other, v_other, p0, p1, p2, p3,
                   ends, his, los, tops,
                   past, change, firsts, first, ys, values, states):
    nb = 4
    n = own.shape[1]
    rho = 1.0 - decay_of(table, n)
    root_inv = lax.rsqrt(rho)
    ordered(place[3], (p0, p1, p2, p3), values)
    ordered_maps(place[0], place[2], own, ((m1, o1), (m2, o2), (m3, o3)), ys)
    state = jnp.zeros((8, n), F32)
    state = lax.fori_loop(0, place[0], lambda k, s: advance(s, ys[k]), state)
    state = lax.fori_loop(0, place[1], lambda k, s: advance(s, xs[k]), state)
    over = state - dot3(split(state), split(other[...])) + v_other[...]
    state = jnp.where(place[2] == 0, state, over)
    at = lax.broadcasted_iota(jnp.int32, (BLOCK, n), 0)
    for b in range(nb):
        states[b] = state
        if b + 1 < nb:
            state = state - dot3(split(state), split(tops[b])) + ends[b]
    for b in range(nb):
        z = values[b] * root_inv
        z = z + jnp.where(at == 0, states[b][0:1], 0.0)
        values[b] = z - dot3(split(z), (his[b], los[b]))
    scan_rows(values, his, los, nb, True)
    for b in range(nb):
        v = values[b]
        before = jnp.where(at == 0, states[b][0:1], pltpu.roll(v, 1, 0)) * rho
        past[b] = before
        change[b] = v - before
        values[b] = v - before
    scan_rows(values, his, los, nb, False)
    back = jnp.zeros((8, n), F32)
    for b in reversed(range(nb)):
        lead = jnp.broadcast_to(values[b][0:1], (8, n))
        firsts[b] = lead
        back = back - dot3(split(back), split(tops[b])) + lead
    first[...] = back


def pair_back_kernel(place, own, far, mine, other, out):
    lead = place[2] == 0
    early_q = jnp.where(lead, own[...], far[...])
    late_q = jnp.where(lead, far[...], own[...])
    early = jnp.where(lead, mine[...], other[...])
    out[...] = early_q + retreat(late_q, early)


def group_back_kernel(place, q0, q1, q2, q3, xs, out, qs):
    n = xs.shape[2]
    ordered(place[1], (q0, q1, q2, q3), qs)
    q = qs[3]
    for k in (2, 1, 0):
        q = qs[k] + retreat(q, xs[k, 0:n, :])
    out[...] = q


def smooth_kernel(place, table, gy0, gy1, gy2, gy3, gxs, far, ys, xs, other,
                  past, change, firsts, his, los, tops,
                  smoothed, high, low, keep, give, gys, values, states, moment):
    nb = 4
    nseg = 4
    ordered(place[0], (gy0, gy1, gy2, gy3), gys)
    n = gy0.shape[1]
    back = jnp.zeros((8, n), F32)

    def over(gs, ms):
        def step(k, s):
            j = nseg - 1 - k
            return gs[j] + retreat(s, ms[j, 0:n, :])

        return step

    back = lax.fori_loop(0, nseg - 1 - place[0], over(gys, ys), back)
    back = lax.fori_loop(0, nseg - 1 - place[1], over(gxs, xs), back)
    back = jnp.where(place[2] == 0, far[...] + retreat(back, other[...]), back)
    at = lax.broadcasted_iota(jnp.int32, (BLOCK, n), 0)
    for b in reversed(range(nb)):
        states[b] = back
        if b:
            back = back - dot3(split(back), split(tops[b])) + firsts[b]
    for b in range(nb):
        s = states[b]
        step = s - dot3(split(s), (his[b], los[b]))
        values[b] = change[b] + jnp.where(at == BLOCK - 1, step[0:1], 0.0)
    scan_rows(values, his, los, nb, False)
    root_inv = lax.rsqrt(1.0 - decay_of(table, n))
    for b in range(nb):
        smoothed[b * BLOCK : (b + 1) * BLOCK, :] = (values[b] + past[b]) * root_inv
    pair = split(smoothed[...])
    high[...], low[...] = pair
    store_packed(moment, dot3(pair, pair, ((0,), (0,))) * (1.0 / (128 * BLOCK)))
    rows = keep.shape[0]
    keep[...] = moment[pl.ds(pl.multiple_of(place[2] * BLOCK, BLOCK), rows), :]
    give[...] = moment[pl.ds(pl.multiple_of((1 - place[2]) * BLOCK, BLOCK), rows), :]


def errors_kernel(panel_of, table, high, low, observed, turned, sums_out):
    nb = 4
    n = sums_out.shape[1]
    series = turned.shape[1]
    coef = turned[...]
    weight = table[0:4, :]
    squares = jnp.zeros((1, series), F32)
    for b in range(nb):
        part = slice(b * BLOCK, (b + 1) * BLOCK)
        miss = observed[part, :].astype(F32) - (dot(high[part, :], coef) + dot(low[part, :], coef))
        squares = squares + jnp.sum(miss * miss, axis=0, keepdims=True) * weight[b : b + 1]
    counts = float(BLOCK) * jnp.sum(weight, axis=0, keepdims=True)
    lane = lax.broadcasted_iota(jnp.int32, (8, n), 1)
    line = lax.broadcasted_iota(jnp.int32, (8, n), 0)
    sums = jnp.zeros((8, n), F32)
    for j in range(series // SER_BLOCK):
        part = slice(j * SER_BLOCK, (j + 1) * SER_BLOCK)
        sq = jnp.sum(squares[:, part], axis=1, keepdims=True)
        ct = jnp.sum(counts[:, part], axis=1, keepdims=True)
        here = lane == panel_of[j]
        sums = sums + jnp.where(here & (line == 0), sq, 0.0) + jnp.where(here & (line == 1), ct, 0.0)
    sums_out[...] = sums


def moment_kernel(place, table, high, low, observed, own_part, far_part, moment):
    nb = 4
    weight = table[0:4, :]
    kept = jnp.concatenate(
        [
            (observed[b * BLOCK : (b + 1) * BLOCK, :].astype(F32) * weight[b : b + 1]).astype(BF16)
            for b in range(nb)
        ],
        axis=0,
    )
    both = ((0,), (0,))
    scale = 1.0 / math.sqrt(128 * BLOCK)
    moment[...] = (dot(high[...], kept, both) + dot(low[...], kept, both)) * scale
    for i in range(16):
        own = moment[pl.ds(pl.multiple_of((2 * i + place[2]) * 8, 8), 8), :]
        far = moment[pl.ds(pl.multiple_of((2 * i + 1 - place[2]) * 8, 8), 8), :]
        for j in range(8):
            own_part[i, 8 * j : 8 * j + 8, :] = own[:, j * 128 : (j + 1) * 128]
            far_part[i, 8 * j : 8 * j + 8, :] = far[:, j * 128 : (j + 1) * 128]


def add_kernel(a, b, out):
    out[...] = a[...] + b[...]


def small_kernel(keep, given, s, s_far, out):
    n = keep.shape[0]
    out[0:n, :] = keep[...] + given[...]
    out[n:, :] = s[...] + s_far[...]


def collect_kernel(arrived, out):
    total = jnp.sum(arrived[...], axis=0)
    for j in range(8):
        out[:, j * 128 : (j + 1) * 128] = total[8 * j : 8 * j + 8]


def variance_kernel(s0, s1, s2, s3, out):
    sums = (s0[...] + s1[...]) + (s2[...] + s3[...])
    out[...] = sums[0:1] / jnp.maximum(sums[1:2], 1.0)


def last_sum_kernel(a, b, c, d, state, sums):
    n = state.shape[0]
    total = (a[...] + b[...]) + (c[...] + d[...])
    state[...] = total[:n]
    sums[...] = total[n:]


def sum_kernel(a, b, c, d, out):
    out[...] = (a[...] + b[...]) + (c[...] + d[...])


def finish_kernel(place, mine, other, out):
    first = jnp.where(place[2] == 0, mine[...], other[...])
    second = jnp.where(place[2] == 0, other[...], mine[...])
    out[...] = unpack(jnp.concatenate([first[0:BLOCK], second], axis=0))


def call(kernel, outs, scratch, *args, smem=1, mib=12):
    shapes = [jax.ShapeDtypeStruct(s, d) for s, d in outs]
    specs = [SMEM] * smem + [VMEM] * (len(args) - smem)
    made = pl.pallas_call(
        kernel,
        out_shape=shapes,
        in_specs=specs,
        out_specs=[VMEM] * len(outs),
        scratch_shapes=[pltpu.VMEM(s, d) for s, d in scratch],
        compiler_params=pltpu.CompilerParams(vmem_limit_bytes=mib << 20),
    )
    return made(*args)


def from_peers(arrays, axis):
    n = lax.axis_size(axis)
    out = [arrays[0]]
    for k in range(1, n):
        out.append(lax.ppermute(arrays[k], axis, [(i, (i + k) % n) for i in range(n)]))
    return out


def gather(array, axis):
    return from_peers([array] * lax.axis_size(axis), axis)


def swap(array, axis):
    return lax.ppermute(array, axis, [(0, 1), (1, 0)])


def step(observed, present, loadings, noise_var, decay_rate, panel_of_block):
    time_rows, series = observed.shape
    width = loadings.shape[1]
    nb = time_rows // BLOCK
    half = width // 2
    ay, ax, ac = TM
    iy, ix, ic, iz = (lax.axis_index(a) for a in (ay, ax, ac, "panel"))
    scalar = lambda *v: jnp.stack([jnp.int32(i) for i in v])
    place = scalar(iy, ix, ic, iz)
    packed = ((width + 8, half), F32)
    map_shape = ((width + 8, width), F32)
    half_shape = ((half + 8, width), F32)
    vec = ((8, width), F32)
    vecs4 = ((4, 8, width), F32)
    maps4 = ((4, width + 8, width), F32)
    rows2 = ((BLOCK, width), F32)
    rows3 = ((nb, BLOCK, width), F32)
    square = ((width, width), F32)
    squares4 = ((nb, width, width), F32)
    powers = ((LEVELS * nb, width, width), BF16)

    noise = noise_var.reshape(1, series)
    grams = call(gram_kernel, [packed] * nb, [], place, present, noise, loadings)
    table, *projs = call(
        project_kernel, [((8, series), F32)] + [rows2] * nb, [],
        place, present, noise, loadings, decay_rate.reshape(1, width), observed,
    )
    grams = from_peers(grams, "panel")
    projs = from_peers(projs, "panel")
    (err,) = call(inverse_kernel, [packed], [square], table, *grams, smem=0)
    errs = gather(err, "panel")
    proj, end = call(end_kernel, [rows2, vec], [square], table, err, *projs, smem=0)
    ends = gather(end, "panel")
    his, los, tops, seg = call(
        powers_kernel, [powers, powers, squares4, square], [squares4], place, *errs
    )
    seg, proj = lax.optimization_barrier((seg, proj))
    seg_far = swap(seg, ac)
    ends, seg_end = call(segment_end_kernel, [vecs4, vec], [], place, tops, *ends)
    end_far = swap(seg_end, ac)
    projs = gather(proj, "panel")
    pair, pair_half = call(pair_kernel, [map_shape, half_shape], [], place, seg, seg_far, seg_end, end_far)
    (turned,) = call(turn_kernel, [((width, series), BF16)], [], loadings, smem=0)
    near = gather(pair_half, ax)[1:]
    group, group_half, xs = call(
        group_kernel, [map_shape, half_shape, maps4], [],
        place, pair, *near, *[swap(m, ac) for m in near],
    )
    near = gather(group_half, ay)[1:]
    past, change, firsts, first, ys = call(
        forward_kernel,
        [rows3, rows3, vecs4, vec, maps4],
        [rows3, vecs4],
        place, table, group, *near, *[swap(m, ac) for m in near],
        xs, seg_far, end_far, *projs, ends, his, los, tops,
    )
    first_far = swap(first, ac)
    (pair_first,) = call(pair_back_kernel, [vec], [], place, first, first_far, seg, seg_far)
    group_first, gxs = call(
        group_back_kernel, [vec, vecs4], [], place, *gather(pair_first, ax), xs
    )
    flat = ((time_rows, width), BF16)
    piece = ((BLOCK + 8, half), F32)
    smoothed, high, low, keep, give = call(
        smooth_kernel,
        [((time_rows, width), F32), flat, flat, piece, piece],
        [vecs4, rows3, vecs4, packed],
        place, table, *gather(group_first, ay), gxs, first_far, ys, xs, seg_far,
        past, change, firsts, his, los, tops,
    )
    given = swap(give, ac)
    line = ((8, half), F32)
    (sums,) = call(errors_kernel, [line], [], panel_of_block, table, high, low, observed, turned)
    tall = ((BLOCK + 16, half), F32)
    (small,) = call(small_kernel, [tall], [], keep, given, sums, swap(sums, ac), smem=0)
    smalls = gather(small, ax)
    part = ((16, 64, half), F32)
    own_part, far_part = call(
        moment_kernel, [part, part], [((width, series), F32)], place, table, high, low, observed
    )
    (spread,) = call(add_kernel, [part], [], own_part, swap(far_part, ac), smem=0)
    arrived = lax.all_to_all(spread, (ay, ax), 0, 0, tiled=True)
    (small,) = call(sum_kernel, [tall], [], *smalls, smem=0)
    smalls = gather(small, ay)
    state, sums = call(last_sum_kernel, [piece, line], [], *smalls, smem=0)
    (state_moment,) = call(finish_kernel, [square], [], place, state, swap(state, ac))
    (var,) = call(variance_kernel, [((1, half), F32)], [], *gather(sums, "panel"), smem=0)
    (loading_moment,) = call(collect_kernel, [((8, series), F32)], [], arrived, smem=0)
    return smoothed, loading_moment, state_moment, var[0, :PANELS]


def solution(mesh):
    finer = Mesh(
        mesh.devices.reshape(4, 4, 2, mesh.shape["panel"]), ("tm_0", "tm_1", "tm_2", "panel")
    )
    in_specs = (P(TM, "panel"), P(TM, "panel"), P("panel", None), P("panel"), P(), P("panel"))
    out_specs = (P(TM, None), P(TM, "panel"), P(), P())
    return jax.shard_map(step, mesh=finer, in_specs=in_specs, out_specs=out_specs, check_vma=False)
```

```python
import math

import jax
import jax.numpy as jnp
from jax import lax
from jax.experimental import pallas as pl
from jax.experimental.pallas import tpu as pltpu
from jax.sharding import Mesh
from jax.sharding import PartitionSpec as P


SER_BLOCK = 128
PANELS = 19
LEVELS = 7
BLOCK = 128
TM = ("tm_0", "tm_1", "tm_2")
F32 = jnp.float32
BF16 = jnp.bfloat16
HIGH = lax.Precision.HIGHEST
VMEM = pl.BlockSpec(memory_space=pltpu.VMEM)
SMEM = pl.BlockSpec(memory_space=pltpu.SMEM)


def split(x):
    hi = x.astype(BF16)
    return hi, (x - hi.astype(F32)).astype(BF16)


def dot(a, b, dims=((1,), (0,))):
    return lax.dot_general(a, b, (dims, ((), ())), preferred_element_type=F32)


def dot3(a, b, dims=((1,), (0,))):
    rows = a[0].shape[0]
    if dims[0] == (1,):
        both = dot(jnp.concatenate(a, axis=0), b[0], dims)
        return (both[:rows] + both[rows:]) + dot(a[0], b[1], dims)
    return dot(a[0], b[0], dims) + (dot(a[0], b[1], dims) + dot(a[1], b[0], dims))


def grid_iota(n, axis):
    return lax.broadcasted_iota(jnp.int32, (n, n), axis)


def eye(n):
    return (grid_iota(n, 0) == grid_iota(n, 1)).astype(F32)


def pack(sym):
    n = sym.shape[0] // 2
    first, corner, second = sym[:n, :n], sym[:n, n:], sym[n:, n:]
    mixed = jnp.where(grid_iota(n, 0) >= grid_iota(n, 1), first, second)
    diag = jnp.sum(second * eye(n), axis=0, keepdims=True)
    return corner, mixed, jnp.broadcast_to(diag, (8, n))


def store_packed(ref, sym):
    n = sym.shape[0] // 2
    corner, mixed, diag = pack(sym)
    ref[0:n, :] = corner
    ref[n : 2 * n, :] = mixed
    ref[2 * n : 2 * n + 8, :] = diag


def unpack(packed):
    n = packed.shape[1]
    corner, mixed, diag = packed[:n], packed[n : 2 * n], packed[2 * n : 2 * n + 1]
    turned = mixed.T
    row, col = grid_iota(n, 0), grid_iota(n, 1)
    first = jnp.where(row >= col, mixed, turned)
    second = jnp.where(row == col, diag, jnp.where(row < col, mixed, turned))
    return jnp.concatenate(
        [jnp.concatenate([first, corner], axis=1), jnp.concatenate([corner.T, second], axis=1)],
        axis=0,
    )


def gram_kernel(place, present, both, loads, table, *outs):
    coef = loads[...]
    series, n = coef.shape
    mask = present[...].astype(F32)
    inv_noise = 1.0 / both[:, 0:series]
    table[0:4, :] = mask
    table[4:5, 0:n] = both[:, series:]
    table[8:12, :] = mask * inv_noise
    high, low = split(coef.T.astype(F32) * inv_noise)
    for k, out in enumerate(outs):
        kept = table[pl.ds(lax.rem(place[3] + k, len(outs)), 1), :].astype(BF16)
        store_packed(out, dot(high * kept, coef) + dot(low * kept, coef))


def project_kernel(place, table, loads, observed, *outs):
    coef = loads[...]
    for k in range(len(outs)):
        b = lax.rem(place[3] + k, len(outs))
        rows = observed[pl.ds(pl.multiple_of(b * BLOCK, BLOCK), BLOCK), :].astype(F32)
        hi, lo = split(rows * table[pl.ds(8 + b, 1), :])
        outs[k][...] = dot(hi, coef) + dot(lo, coef)


def turn_kernel(loads, out):
    out[...] = loads[...].astype(F32).T.astype(BF16)


def decay_of(table, n):
    return table[4:5, 0:n]


def inverse_kernel(table, g0, g1, g2, g3, out, guess):
    gram = unpack((g0[...] + g1[...]) + (g2[...] + g3[...]))
    n = gram.shape[0]
    ident = eye(n)
    whole = ident + gram
    size = jnp.max(jnp.sum(jnp.abs(gram), axis=1, keepdims=True))
    frob = jnp.sqrt(jnp.max(jnp.sum(jnp.sum(gram * gram, axis=1, keepdims=True), axis=0, keepdims=True)))
    top = 1.0 + jnp.minimum(size, frob) * 1.001
    scale = 2.0 / (1.0 + top)
    start = (top - 1.0) / (top + 1.0)
    guess[...] = (2.0 * scale) * ident - (scale * scale) * whole

    def improve(x):
        rest = 2.0 * ident - jnp.dot(whole, x, precision=HIGH, preferred_element_type=F32)
        return jnp.dot(x, rest, precision=HIGH, preferred_element_type=F32)

    def body(err):
        guess[...] = improve(guess[...])
        return err * err

    def quick(err):
        x = guess[...]
        pair = split(x)
        guess[...] = 2.0 * x - dot3(pair, split(dot3(split(whole), pair)))
        return err * err

    err = lax.while_loop(lambda e: (e > 1e-4) & (top < 8.0), quick, start * start)
    lax.while_loop(lambda e: e > 0.99e-8, body, err)
    inverse = guess[...]
    gain = jnp.dot(gram, inverse, precision=HIGH, preferred_element_type=F32)
    gain = 0.5 * (gain + gain.T)
    rho = 1.0 - decay_of(table, n)
    root = jnp.sqrt(rho)
    root_down = jnp.sum(ident * root, axis=1, keepdims=True)
    store_packed(out, ident * (1.0 - rho) + gain * root * root_down)


def shifted(rows, offset, ahead):
    n = rows.shape[0]
    at = lax.broadcasted_iota(jnp.int32, rows.shape, 0)
    if ahead:
        return jnp.where(at >= offset, pltpu.roll(rows, offset, 0), 0.0)
    return jnp.where(at < n - offset, pltpu.roll(rows, n - offset, 0), 0.0)


def end_kernel(table, packed, p0, p1, p2, p3, total, out, err_ref):
    proj = (p0[...] + p1[...]) + (p2[...] + p3[...])
    total[...] = proj
    z = proj * lax.rsqrt(1.0 - decay_of(table, proj.shape[1]))
    err_ref[...] = unpack(packed[...])
    v = z - dot3(split(z), split(err_ref[...]))
    for level in range(LEVELS):
        pair = split(err_ref[...])
        v = v + shifted(v - dot3(split(v), pair), 1 << level, True)
        if level + 1 < LEVELS:
            err_ref[...] = 2.0 * err_ref[...] - dot3(pair, pair)
    out[...] = jnp.broadcast_to(v[BLOCK - 1 :], out.shape)


def powers_kernel(place, e0, e1, e2, e3, his, los, tops, whole, errs):
    nb = 4
    for k, e in enumerate((e0, e1, e2, e3)):
        errs[lax.rem(place[3] + nb - k, nb)] = unpack(e[...])

    def square(level, carry):
        for b in range(nb):
            err = errs[b]
            pair = split(err)
            his[level * nb + b] = pair[0]
            los[level * nb + b] = pair[1]
            errs[b] = 2.0 * err - dot3(pair, pair)
        return carry

    lax.fori_loop(0, LEVELS, square, 0)
    total = errs[0]
    tops[0] = total
    for b in range(1, nb):
        err = errs[b]
        tops[b] = err
        total = total + err - dot3(split(total), split(err))
    whole[...] = total


def segment_end_kernel(place, tops, v0, v1, v2, v3, ends, out):
    nb = 4
    ordered(place[3], (v0, v1, v2, v3), ends)
    end = ends[0]
    for b in range(1, nb):
        end = end - dot3(split(end), split(tops[b])) + ends[b]
    out[...] = end


def join(maps):
    n = maps[0].shape[1]
    total, end = maps[0][:n], maps[0][n:]
    for m in maps[1:]:
        err = m[:n]
        pair = split(err)
        end = end - dot3(split(end), pair) + m[n:]
        total = total + err - dot3(split(total), pair)
    return total, end


def store_map(total, end, core, out, half):
    n = total.shape[1]
    h = n // 2
    out[0:n, :] = total
    out[n:, :] = end
    half[0:h, :] = out[pl.ds(pl.multiple_of(core * h, h), h), :]
    half[h:, :] = end


def pair_kernel(place, mine, other, v_mine, v_other, out, half):
    own, far, v_own, v_far = mine[...], other[...], v_mine[...], v_other[...]
    first = place[2] == 0
    total = jnp.where(first, own, far)
    err = jnp.where(first, far, own)
    pair = split(err)
    end = jnp.where(first, v_own, v_far)
    end = end - dot3(split(end), pair) + jnp.where(first, v_far, v_own)
    total = total + err - dot3(split(total), pair)
    store_map(total, end, place[2], out, half)


def ordered(place, refs, scratch):
    for k, r in enumerate(refs):
        scratch[lax.rem(place + len(refs) - k, len(refs))] = r[...]


def ordered_maps(place, core, own, halves, maps):
    n = own.shape[1]
    h = n // 2
    maps[place] = own[...]
    for k, (mine, other) in enumerate(halves):
        at = lax.rem(place + 3 - k, 4)
        maps[at, pl.ds(pl.multiple_of(core * h, h), h), :] = mine[0:h, :]
        maps[at, pl.ds(pl.multiple_of((1 - core) * h, h), h), :] = other[0:h, :]
        maps[at, n:, :] = mine[h:, :]


def group_kernel(place, own, m1, m2, m3, o1, o2, o3, out, half, maps):
    ordered_maps(place[1], place[2], own, ((m1, o1), (m2, o2), (m3, o3)), maps)
    total, end = join([maps[k] for k in range(4)])
    store_map(total, end, place[2], out, half)


def advance(state, m):
    n = state.shape[1]
    return state - dot3(split(state), split(m[:n])) + m[n:]


def retreat(state, err):
    return state - dot3(split(state), split(err), ((1,), (1,)))


def scan_rows(values, his, los, nb, ahead):
    for level in range(LEVELS):
        for b in range(nb):
            v = values[b]
            pair = (his[level * nb + b], los[level * nb + b])
            values[b] = v + shifted(v - dot3(split(v), pair), 1 << level, ahead)


def prefix_kernel(place, xs, other, v_other, tops, ends, starts, rests):
    nb = 4
    n = other.shape[1]

    def after(total, end, err, v):
        pair = split(err)
        return total + err - dot3(split(total), pair), end - dot3(split(end), pair) + v

    starts[0] = jnp.zeros((n + 8, n), F32)

    def into(k, carry):
        starts[0, 0:n, :], starts[0, n:, :] = after(
            starts[0, 0:n, :], starts[0, n:, :], xs[k, 0:n, :], xs[k, n:, :]
        )
        return carry

    lax.fori_loop(0, place[1], into, 0)

    @pl.when(place[2] == 1)
    def _():
        starts[0, 0:n, :], starts[0, n:, :] = after(
            starts[0, 0:n, :], starts[0, n:, :], other[...], v_other[...]
        )

    def before(err, total):
        return total + err - dot3(split(err), split(total))

    rests[nb - 1] = jnp.zeros((n, n), F32)

    def back(k, carry):
        rests[nb - 1] = before(xs[3 - k, 0:n, :], rests[nb - 1])
        return carry

    lax.fori_loop(0, 3 - place[1], back, 0)

    @pl.when(place[2] == 0)
    def _():
        rests[nb - 1] = before(other[...], rests[nb - 1])

    def blocks(b, carry):
        starts[b + 1, 0:n, :], starts[b + 1, n:, :] = after(
            starts[b, 0:n, :], starts[b, n:, :], tops[b], ends[b]
        )
        late = nb - 1 - b
        rests[late - 1] = before(tops[late], rests[late])
        return carry

    lax.fori_loop(0, nb - 1, blocks, 0)


def suffix_kernel(place, qs, xs, far, other, tops, firsts, offsets):
    nb = 4
    n = other.shape[1]

    def over(k, s):
        j = 3 - k
        return qs[j] + retreat(s, xs[j, 0:n, :])

    back = lax.fori_loop(0, 3 - place[1], over, jnp.zeros((8, n), F32))
    back = jnp.where(place[2] == 0, far[...] + retreat(back, other[...]), back)
    for b in reversed(range(nb)):
        offsets[b] = back
        if b:
            back = back - dot3(split(back), split(tops[b])) + firsts[b]


def forward_kernel(place, table, own, m1, m2, m3, o1, o2, o3, starts, p0, p1, p2, p3,
                   his, los, tops,
                   past, change, firsts, first, ys, values, states):
    nb = 4
    n = own.shape[1]
    rho = 1.0 - decay_of(table, n)
    root_inv = lax.rsqrt(rho)
    ordered(place[3], (p0, p1, p2, p3), values)
    ordered_maps(place[0], place[2], own, ((m1, o1), (m2, o2), (m3, o3)), ys)
    state = jnp.zeros((8, n), F32)
    state = lax.fori_loop(0, place[0], lambda k, s: advance(s, ys[k]), state)
    at = lax.broadcasted_iota(jnp.int32, (BLOCK, n), 0)
    for b in range(nb):
        states[b] = advance(state, starts[b])
    for b in range(nb):
        z = values[b] * root_inv
        z = z + jnp.where(at == 0, states[b][0:1], 0.0)
        values[b] = z - dot3(split(z), (his[b], los[b]))
    scan_rows(values, his, los, nb, True)
    for b in range(nb):
        v = values[b]
        before = jnp.where(at == 0, states[b][0:1], pltpu.roll(v, 1, 0)) * rho
        past[b] = before
        change[b] = v - before
        values[b] = v - before
    scan_rows(values, his, los, nb, False)
    back = jnp.zeros((8, n), F32)
    for b in reversed(range(nb)):
        lead = jnp.broadcast_to(values[b][0:1], (8, n))
        firsts[b] = lead
        back = back - dot3(split(back), split(tops[b])) + lead
    first[...] = back


def pair_back_kernel(place, own, far, mine, other, out):
    lead = place[2] == 0
    early_q = jnp.where(lead, own[...], far[...])
    late_q = jnp.where(lead, far[...], own[...])
    early = jnp.where(lead, mine[...], other[...])
    out[...] = early_q + retreat(late_q, early)


def group_back_kernel(place, q0, q1, q2, q3, xs, out, qs):
    n = xs.shape[2]
    ordered(place[1], (q0, q1, q2, q3), qs)
    q = qs[3]
    for k in (2, 1, 0):
        q = qs[k] + retreat(q, xs[k, 0:n, :])
    out[...] = q


def smooth_kernel(place, table, gy0, gy1, gy2, gy3, ys, rests, offsets,
                  past, change, his, los,
                  smoothed, high, low, keep, give, gys, values, moment):
    nb = 4
    nseg = 4
    ordered(place[0], (gy0, gy1, gy2, gy3), gys)
    n = gy0.shape[1]
    back = jnp.zeros((8, n), F32)

    def over(k, s):
        j = nseg - 1 - k
        return gys[j] + retreat(s, ys[j, 0:n, :])

    back = lax.fori_loop(0, nseg - 1 - place[0], over, back)
    at = lax.broadcasted_iota(jnp.int32, (BLOCK, n), 0)
    for b in range(nb):
        s = offsets[b] + retreat(back, rests[b])
        step = s - dot3(split(s), (his[b], los[b]))
        values[b] = change[b] + jnp.where(at == BLOCK - 1, step[0:1], 0.0)
    scan_rows(values, his, los, nb, False)
    root_inv = lax.rsqrt(1.0 - decay_of(table, n))
    for b in range(nb):
        smoothed[b * BLOCK : (b + 1) * BLOCK, :] = (values[b] + past[b]) * root_inv
    pair = split(smoothed[...])
    high[...], low[...] = pair
    store_packed(moment, dot3(pair, pair, ((0,), (0,))) * (1.0 / (128 * BLOCK)))
    rows = keep.shape[0]
    keep[...] = moment[pl.ds(pl.multiple_of(place[2] * BLOCK, BLOCK), rows), :]
    give[...] = moment[pl.ds(pl.multiple_of((1 - place[2]) * BLOCK, BLOCK), rows), :]


def errors_kernel(panel_of, table, high, low, observed, turned, sums_out):
    nb = 4
    n = sums_out.shape[1]
    series = turned.shape[1]
    coef = turned[...]
    weight = table[0:4, :]
    squares = jnp.zeros((1, series), F32)
    for b in range(nb):
        part = slice(b * BLOCK, (b + 1) * BLOCK)
        miss = observed[part, :].astype(F32) - (dot(high[part, :], coef) + dot(low[part, :], coef))
        squares = squares + jnp.sum(miss * miss, axis=0, keepdims=True) * weight[b : b + 1]
    counts = float(BLOCK) * jnp.sum(weight, axis=0, keepdims=True)
    lane = lax.broadcasted_iota(jnp.int32, (8, n), 1)
    line = lax.broadcasted_iota(jnp.int32, (8, n), 0)
    sums = jnp.zeros((8, n), F32)
    for j in range(series // SER_BLOCK):
        part = slice(j * SER_BLOCK, (j + 1) * SER_BLOCK)
        sq = jnp.sum(squares[:, part], axis=1, keepdims=True)
        ct = jnp.sum(counts[:, part], axis=1, keepdims=True)
        here = lane == panel_of[j]
        sums = sums + jnp.where(here & (line == 0), sq, 0.0) + jnp.where(here & (line == 1), ct, 0.0)
    sums_out[...] = sums


def moment_kernel(place, table, high, low, observed, own_part, far_part, moment):
    nb = 4
    weight = table[0:4, :]
    kept = jnp.concatenate(
        [
            (observed[b * BLOCK : (b + 1) * BLOCK, :].astype(F32) * weight[b : b + 1]).astype(BF16)
            for b in range(nb)
        ],
        axis=0,
    )
    both = ((0,), (0,))
    scale = 1.0 / math.sqrt(128 * BLOCK)
    moment[...] = (dot(high[...], kept, both) + dot(low[...], kept, both)) * scale
    for i in range(16):
        own = moment[pl.ds(pl.multiple_of((2 * i + place[2]) * 8, 8), 8), :]
        far = moment[pl.ds(pl.multiple_of((2 * i + 1 - place[2]) * 8, 8), 8), :]
        for j in range(8):
            own_part[i, 8 * j : 8 * j + 8, :] = own[:, j * 128 : (j + 1) * 128]
            far_part[i, 8 * j : 8 * j + 8, :] = far[:, j * 128 : (j + 1) * 128]


def add_kernel(a, b, out):
    out[...] = a[...] + b[...]


def small_kernel(keep, given, s, s_far, out):
    n = keep.shape[0]
    out[0:n, :] = keep[...] + given[...]
    out[n:, :] = s[...] + s_far[...]


def collect_kernel(arrived, out):
    total = jnp.sum(arrived[...], axis=0)
    for j in range(8):
        out[:, j * 128 : (j + 1) * 128] = total[8 * j : 8 * j + 8]


def variance_kernel(s0, s1, s2, s3, out):
    sums = (s0[...] + s1[...]) + (s2[...] + s3[...])
    out[...] = sums[0:1] / jnp.maximum(sums[1:2], 1.0)


def last_sum_kernel(a, b, c, d, state, sums):
    n = state.shape[0]
    total = (a[...] + b[...]) + (c[...] + d[...])
    state[...] = total[:n]
    sums[...] = total[n:]


def sum_kernel(a, b, c, d, out):
    out[...] = (a[...] + b[...]) + (c[...] + d[...])


def finish_kernel(place, mine, other, out):
    first = jnp.where(place[2] == 0, mine[...], other[...])
    second = jnp.where(place[2] == 0, other[...], mine[...])
    out[...] = unpack(jnp.concatenate([first[0:BLOCK], second], axis=0))


def call(kernel, outs, scratch, *args, smem=1, mib=12):
    shapes = [jax.ShapeDtypeStruct(s, d) for s, d in outs]
    specs = [SMEM] * smem + [VMEM] * (len(args) - smem)
    made = pl.pallas_call(
        kernel,
        out_shape=shapes,
        in_specs=specs,
        out_specs=[VMEM] * len(outs),
        scratch_shapes=[pltpu.VMEM(s, d) for s, d in scratch],
        compiler_params=pltpu.CompilerParams(vmem_limit_bytes=mib << 20),
    )
    return made(*args)


def from_peers(arrays, axis):
    n = lax.axis_size(axis)
    out = [arrays[0]]
    for k in range(1, n):
        out.append(lax.ppermute(arrays[k], axis, [(i, (i + k) % n) for i in range(n)]))
    return out


def gather(array, axis):
    return from_peers([array] * lax.axis_size(axis), axis)


def swap(array, axis):
    return lax.ppermute(array, axis, [(0, 1), (1, 0)])


def step(observed, present, loadings, noise_var, decay_rate, panel_of_block):
    time_rows, series = observed.shape
    width = loadings.shape[1]
    nb = time_rows // BLOCK
    half = width // 2
    ay, ax, ac = TM
    iy, ix, ic, iz = (lax.axis_index(a) for a in (ay, ax, ac, "panel"))
    scalar = lambda *v: jnp.stack([jnp.int32(i) for i in v])
    place = scalar(iy, ix, ic, iz)
    packed = ((width + 8, half), F32)
    map_shape = ((width + 8, width), F32)
    half_shape = ((half + 8, width), F32)
    vec = ((8, width), F32)
    vecs4 = ((4, 8, width), F32)
    maps4 = ((4, width + 8, width), F32)
    rows2 = ((BLOCK, width), F32)
    rows3 = ((nb, BLOCK, width), F32)
    square = ((width, width), F32)
    squares4 = ((nb, width, width), F32)
    powers = ((LEVELS * nb, width, width), BF16)

    both = jnp.concatenate([noise_var, decay_rate]).reshape(1, series + width)
    table, *grams = call(
        gram_kernel, [((16, series), F32)] + [packed] * nb, [], place, present, both, loadings
    )
    projs = call(project_kernel, [rows2] * nb, [], place, table, loadings, observed)
    grams = from_peers(grams, "panel")
    projs = from_peers(projs, "panel")
    (err,) = call(inverse_kernel, [packed], [square], table, *grams, smem=0)
    errs = gather(err, "panel")
    proj, end = call(end_kernel, [rows2, vec], [square], table, err, *projs, smem=0)
    ends = gather(end, "panel")
    his, los, tops, seg = call(
        powers_kernel, [powers, powers, squares4, square], [squares4], place, *errs
    )
    seg, proj = lax.optimization_barrier((seg, proj))
    seg_far = swap(seg, ac)
    ends, seg_end = call(segment_end_kernel, [vecs4, vec], [], place, tops, *ends)
    end_far = swap(seg_end, ac)
    projs = gather(proj, "panel")
    pair, pair_half = call(pair_kernel, [map_shape, half_shape], [], place, seg, seg_far, seg_end, end_far)
    (turned,) = call(turn_kernel, [((width, series), BF16)], [], loadings, smem=0)
    near = gather(pair_half, ax)[1:]
    group, group_half, xs = call(
        group_kernel, [map_shape, half_shape, maps4], [],
        place, pair, *near, *[swap(m, ac) for m in near],
    )
    near = gather(group_half, ay)[1:]
    starts, rests = call(
        prefix_kernel, [maps4, squares4], [], place, xs, seg_far, end_far, tops, ends
    )
    past, change, firsts, first, ys = call(
        forward_kernel,
        [rows3, rows3, vecs4, vec, maps4],
        [rows3, vecs4],
        place, table, group, *near, *[swap(m, ac) for m in near],
        starts, *projs, his, los, tops,
    )
    first_far = swap(first, ac)
    (pair_first,) = call(pair_back_kernel, [vec], [], place, first, first_far, seg, seg_far)
    group_first, gxs = call(
        group_back_kernel, [vec, vecs4], [], place, *gather(pair_first, ax), xs
    )
    flat = ((time_rows, width), BF16)
    piece = ((BLOCK + 8, half), F32)
    firsts_y = gather(group_first, ay)
    (offsets,) = call(suffix_kernel, [vecs4], [], place, gxs, xs, first_far, seg_far, tops, firsts)
    smoothed, high, low, keep, give = call(
        smooth_kernel,
        [((time_rows, width), F32), flat, flat, piece, piece],
        [vecs4, rows3, packed],
        place, table, *firsts_y, ys, rests, offsets, past, change, his, los,
    )
    given = swap(give, ac)
    line = ((8, half), F32)
    (sums,) = call(errors_kernel, [line], [], panel_of_block, table, high, low, observed, turned)
    tall = ((BLOCK + 16, half), F32)
    (small,) = call(small_kernel, [tall], [], keep, given, sums, swap(sums, ac), smem=0)
    smalls = gather(small, ax)
    part = ((16, 64, half), F32)
    own_part, far_part = call(
        moment_kernel, [part, part], [((width, series), F32)], place, table, high, low, observed
    )
    (spread,) = call(add_kernel, [part], [], own_part, swap(far_part, ac), smem=0)
    arrived = lax.all_to_all(spread, (ay, ax), 0, 0, tiled=True)
    (small,) = call(sum_kernel, [tall], [], *smalls, smem=0)
    smalls = gather(small, ay)
    state, sums = call(last_sum_kernel, [piece, line], [], *smalls, smem=0)
    (state_moment,) = call(finish_kernel, [square], [], place, state, swap(state, ac))
    (var,) = call(variance_kernel, [((1, half), F32)], [], *gather(sums, "panel"), smem=0)
    (loading_moment,) = call(collect_kernel, [((8, series), F32)], [], arrived, smem=0)
    return smoothed, loading_moment, state_moment, var[0, :PANELS]


def solution(mesh):
    finer = Mesh(
        mesh.devices.reshape(4, 4, 2, mesh.shape["panel"]), ("tm_0", "tm_1", "tm_2", "panel")
    )
    in_specs = (P(TM, "panel"), P(TM, "panel"), P("panel", None), P("panel"), P(), P("panel"))
    out_specs = (P(TM, None), P(TM, "panel"), P(), P())
    return jax.shard_map(step, mesh=finer, in_specs=in_specs, out_specs=out_specs, check_vma=False)
```

```python
import math

import jax
import jax.numpy as jnp
from jax import lax
from jax.experimental import pallas as pl
from jax.experimental.pallas import tpu as pltpu
from jax.sharding import Mesh
from jax.sharding import PartitionSpec as P


SER_BLOCK = 128
PANELS = 19
LEVELS = 7
BLOCK = 128
TM = ("tm_0", "tm_1", "tm_2")
F32 = jnp.float32
BF16 = jnp.bfloat16
HIGH = lax.Precision.HIGHEST
VMEM = pl.BlockSpec(memory_space=pltpu.VMEM)
SMEM = pl.BlockSpec(memory_space=pltpu.SMEM)


def split(x):
    hi = x.astype(BF16)
    return hi, (x - hi.astype(F32)).astype(BF16)


def dot(a, b, dims=((1,), (0,))):
    return lax.dot_general(a, b, (dims, ((), ())), preferred_element_type=F32)


def dot3(a, b, dims=((1,), (0,))):
    rows = a[0].shape[0]
    if dims[0] == (1,):
        both = dot(jnp.concatenate(a, axis=0), b[0], dims)
        return (both[:rows] + both[rows:]) + dot(a[0], b[1], dims)
    return dot(a[0], b[0], dims) + (dot(a[0], b[1], dims) + dot(a[1], b[0], dims))


def grid_iota(n, axis):
    return lax.broadcasted_iota(jnp.int32, (n, n), axis)


def eye(n):
    return (grid_iota(n, 0) == grid_iota(n, 1)).astype(F32)


def pack(sym):
    n = sym.shape[0] // 2
    first, corner, second = sym[:n, :n], sym[:n, n:], sym[n:, n:]
    mixed = jnp.where(grid_iota(n, 0) >= grid_iota(n, 1), first, second)
    diag = jnp.sum(second * eye(n), axis=0, keepdims=True)
    return corner, mixed, jnp.broadcast_to(diag, (8, n))


def store_packed(ref, sym):
    n = sym.shape[0] // 2
    corner, mixed, diag = pack(sym)
    ref[0:n, :] = corner
    ref[n : 2 * n, :] = mixed
    ref[2 * n : 2 * n + 8, :] = diag


def unpack(packed):
    n = packed.shape[1]
    corner, mixed, diag = packed[:n], packed[n : 2 * n], packed[2 * n : 2 * n + 1]
    turned = mixed.T
    row, col = grid_iota(n, 0), grid_iota(n, 1)
    first = jnp.where(row >= col, mixed, turned)
    second = jnp.where(row == col, diag, jnp.where(row < col, mixed, turned))
    return jnp.concatenate(
        [jnp.concatenate([first, corner], axis=1), jnp.concatenate([corner.T, second], axis=1)],
        axis=0,
    )


def gram_kernel(place, present, both, loads, table, kept_loads, *outs):
    coef = loads[...]
    kept_loads[...] = coef
    series, n = coef.shape
    mask = present[...].astype(F32)
    inv_noise = 1.0 / both[:, 0:series]
    table[0:4, :] = mask
    table[4:5, 0:n] = both[:, series:]
    table[8:12, :] = mask * inv_noise
    high, low = split(coef.T.astype(F32) * inv_noise)
    for k, out in enumerate(outs):
        kept = table[pl.ds(lax.rem(place[3] + k, len(outs)), 1), :].astype(BF16)
        store_packed(out, dot(high * kept, coef) + dot(low * kept, coef))


def project_kernel(place, table, loads, observed, *outs):
    coef = loads[...]
    for k in range(len(outs)):
        b = lax.rem(place[3] + k, len(outs))
        rows = observed[pl.ds(pl.multiple_of(b * BLOCK, BLOCK), BLOCK), :].astype(F32)
        hi, lo = split(rows * table[pl.ds(8 + b, 1), :])
        outs[k][...] = dot(hi, coef) + dot(lo, coef)


def turn_kernel(loads, out):
    out[...] = loads[...].astype(F32).T.astype(BF16)


def decay_of(table, n):
    return table[4:5, 0:n]


def inverse_kernel(table, g0, g1, g2, g3, out, guess):
    gram = unpack((g0[...] + g1[...]) + (g2[...] + g3[...]))
    n = gram.shape[0]
    ident = eye(n)
    whole = ident + gram
    size = jnp.max(jnp.sum(jnp.abs(gram), axis=1, keepdims=True))
    frob = jnp.sqrt(jnp.max(jnp.sum(jnp.sum(gram * gram, axis=1, keepdims=True), axis=0, keepdims=True)))
    top = 1.0 + jnp.minimum(size, frob) * 1.001
    scale = 2.0 / (1.0 + top)
    start = (top - 1.0) / (top + 1.0)
    guess[...] = (2.0 * scale) * ident - (scale * scale) * whole

    def improve(x):
        rest = 2.0 * ident - jnp.dot(whole, x, precision=HIGH, preferred_element_type=F32)
        return jnp.dot(x, rest, precision=HIGH, preferred_element_type=F32)

    def body(err):
        guess[...] = improve(guess[...])
        return err * err

    def quick(err):
        x = guess[...]
        pair = split(x)
        guess[...] = 2.0 * x - dot3(pair, split(dot3(split(whole), pair)))
        return err * err

    err = lax.while_loop(lambda e: (e > 2e-4) & (top < 8.0), quick, start * start)
    lax.while_loop(lambda e: e > 3.9e-8, body, err)
    inverse = guess[...]
    gain = jnp.dot(gram, inverse, precision=HIGH, preferred_element_type=F32)
    gain = 0.5 * (gain + gain.T)
    rho = 1.0 - decay_of(table, n)
    root = jnp.sqrt(rho)
    root_down = jnp.sum(ident * root, axis=1, keepdims=True)
    store_packed(out, ident * (1.0 - rho) + gain * root * root_down)


def shifted(rows, offset, ahead):
    n = rows.shape[0]
    at = lax.broadcasted_iota(jnp.int32, rows.shape, 0)
    if ahead:
        return jnp.where(at >= offset, pltpu.roll(rows, offset, 0), 0.0)
    return jnp.where(at < n - offset, pltpu.roll(rows, n - offset, 0), 0.0)


def end_kernel(table, packed, p0, p1, p2, p3, total, out, err_ref):
    proj = (p0[...] + p1[...]) + (p2[...] + p3[...])
    total[...] = proj
    z = proj * lax.rsqrt(1.0 - decay_of(table, proj.shape[1]))
    err_ref[...] = unpack(packed[...])
    v = z - dot3(split(z), split(err_ref[...]))
    for level in range(LEVELS):
        pair = split(err_ref[...])
        v = v + shifted(v - dot3(split(v), pair), 1 << level, True)
        if level + 1 < LEVELS:
            err_ref[...] = 2.0 * err_ref[...] - dot3(pair, pair)
    out[...] = jnp.broadcast_to(v[BLOCK - 1 :], out.shape)


def powers_kernel(place, e0, e1, e2, e3, his, los, tops, whole, errs):
    nb = 4
    for k, e in enumerate((e0, e1, e2, e3)):
        errs[lax.rem(place[3] + nb - k, nb)] = unpack(e[...])

    def square(level):
        for b in range(nb):
            err = errs[b]
            pair = split(err)
            his[level * nb + b] = pair[0]
            los[level * nb + b] = pair[1]
            errs[b] = 2.0 * err - dot3(pair, pair)

    def squares(k, carry):
        square(2 * k)
        square(2 * k + 1)
        return carry

    lax.fori_loop(0, LEVELS // 2, squares, 0)
    square(LEVELS - 1)
    total = errs[0]
    tops[0] = total
    for b in range(1, nb):
        err = errs[b]
        tops[b] = err
        total = total + err - dot3(split(total), split(err))
    whole[...] = total


def segment_end_kernel(place, tops, v0, v1, v2, v3, ends, out):
    nb = 4
    ordered(place[3], (v0, v1, v2, v3), ends)
    end = ends[0]
    for b in range(1, nb):
        end = end - dot3(split(end), split(tops[b])) + ends[b]
    out[...] = end


def join(maps):
    n = maps[0].shape[1]
    total, end = maps[0][:n], maps[0][n:]
    for m in maps[1:]:
        err = m[:n]
        pair = split(err)
        end = end - dot3(split(end), pair) + m[n:]
        total = total + err - dot3(split(total), pair)
    return total, end


def store_map(total, end, core, out, half):
    n = total.shape[1]
    h = n // 2
    out[0:n, :] = total
    out[n:, :] = end
    half[0:h, :] = out[pl.ds(pl.multiple_of(core * h, h), h), :]
    half[h:, :] = end


def pair_kernel(place, mine, other, v_mine, v_other, out, half):
    own, far, v_own, v_far = mine[...], other[...], v_mine[...], v_other[...]
    first = place[2] == 0
    total = jnp.where(first, own, far)
    err = jnp.where(first, far, own)
    pair = split(err)
    end = jnp.where(first, v_own, v_far)
    end = end - dot3(split(end), pair) + jnp.where(first, v_far, v_own)
    total = total + err - dot3(split(total), pair)
    store_map(total, end, place[2], out, half)


def ordered(place, refs, scratch):
    for k, r in enumerate(refs):
        scratch[lax.rem(place + len(refs) - k, len(refs))] = r[...]


def ordered_maps(place, core, own, halves, maps):
    n = own.shape[1]
    h = n // 2
    maps[place] = own[...]
    for k, (mine, other) in enumerate(halves):
        at = lax.rem(place + 3 - k, 4)
        maps[at, pl.ds(pl.multiple_of(core * h, h), h), :] = mine[0:h, :]
        maps[at, pl.ds(pl.multiple_of((1 - core) * h, h), h), :] = other[0:h, :]
        maps[at, n:, :] = mine[h:, :]


def group_kernel(place, own, m1, m2, m3, o1, o2, o3, out, half, maps):
    ordered_maps(place[1], place[2], own, ((m1, o1), (m2, o2), (m3, o3)), maps)
    total, end = join([maps[k] for k in range(4)])
    store_map(total, end, place[2], out, half)


def advance(state, m):
    n = state.shape[1]
    return state - dot3(split(state), split(m[:n])) + m[n:]


def retreat(state, err):
    return state - dot3(split(state), split(err), ((1,), (1,)))


def scan_rows(values, his, los, nb, ahead):
    for level in range(LEVELS):
        for b in range(nb):
            v = values[b]
            pair = (his[level * nb + b], los[level * nb + b])
            values[b] = v + shifted(v - dot3(split(v), pair), 1 << level, ahead)


def prefix_kernel(place, xs, other, v_other, tops, ends, starts, rests):
    nb = 4
    n = other.shape[1]

    def after(total, end, err, v):
        pair = split(err)
        return total + err - dot3(split(total), pair), end - dot3(split(end), pair) + v

    starts[0] = jnp.zeros((n + 8, n), F32)

    def into(k, carry):
        starts[0, 0:n, :], starts[0, n:, :] = after(
            starts[0, 0:n, :], starts[0, n:, :], xs[k, 0:n, :], xs[k, n:, :]
        )
        return carry

    lax.fori_loop(0, place[1], into, 0)

    @pl.when(place[2] == 1)
    def _():
        starts[0, 0:n, :], starts[0, n:, :] = after(
            starts[0, 0:n, :], starts[0, n:, :], other[...], v_other[...]
        )

    def before(err, total):
        return total + err - dot3(split(err), split(total))

    rests[nb - 1] = jnp.zeros((n, n), F32)

    def back(k, carry):
        rests[nb - 1] = before(xs[3 - k, 0:n, :], rests[nb - 1])
        return carry

    lax.fori_loop(0, 3 - place[1], back, 0)

    @pl.when(place[2] == 0)
    def _():
        rests[nb - 1] = before(other[...], rests[nb - 1])

    def blocks(b, carry):
        starts[b + 1, 0:n, :], starts[b + 1, n:, :] = after(
            starts[b, 0:n, :], starts[b, n:, :], tops[b], ends[b]
        )
        late = nb - 1 - b
        rests[late - 1] = before(tops[late], rests[late])
        return carry

    lax.fori_loop(0, nb - 1, blocks, 0)


def suffix_kernel(place, qs, xs, far, other, tops, firsts, offsets):
    nb = 4
    n = other.shape[1]

    def over(k, s):
        j = 3 - k
        return qs[j] + retreat(s, xs[j, 0:n, :])

    back = lax.fori_loop(0, 3 - place[1], over, jnp.zeros((8, n), F32))
    back = jnp.where(place[2] == 0, far[...] + retreat(back, other[...]), back)
    for b in reversed(range(nb)):
        offsets[b] = back
        if b:
            back = back - dot3(split(back), split(tops[b])) + firsts[b]


def forward_kernel(place, table, own, m1, m2, m3, o1, o2, o3, starts, p0, p1, p2, p3,
                   his, los, tops,
                   past, change, firsts, first, ys, values, states):
    nb = 4
    n = own.shape[1]
    rho = 1.0 - decay_of(table, n)
    root_inv = lax.rsqrt(rho)
    ordered(place[3], (p0, p1, p2, p3), values)
    ordered_maps(place[0], place[2], own, ((m1, o1), (m2, o2), (m3, o3)), ys)
    state = jnp.zeros((8, n), F32)
    state = lax.fori_loop(0, place[0], lambda k, s: advance(s, ys[k]), state)
    at = lax.broadcasted_iota(jnp.int32, (BLOCK, n), 0)
    for b in range(nb):
        states[b] = advance(state, starts[b])
    for b in range(nb):
        z = values[b] * root_inv
        z = z + jnp.where(at == 0, states[b][0:1], 0.0)
        values[b] = z - dot3(split(z), (his[b], los[b]))
    scan_rows(values, his, los, nb, True)
    for b in range(nb):
        v = values[b]
        before = jnp.where(at == 0, states[b][0:1], pltpu.roll(v, 1, 0)) * rho
        past[b] = before
        change[b] = v - before
        values[b] = v - before
    scan_rows(values, his, los, nb, False)
    back = jnp.zeros((8, n), F32)
    for b in reversed(range(nb)):
        lead = jnp.broadcast_to(values[b][0:1], (8, n))
        firsts[b] = lead
        back = back - dot3(split(back), split(tops[b])) + lead
    first[...] = back


def pair_back_kernel(place, own, far, mine, other, out):
    lead = place[2] == 0
    early_q = jnp.where(lead, own[...], far[...])
    late_q = jnp.where(lead, far[...], own[...])
    early = jnp.where(lead, mine[...], other[...])
    out[...] = early_q + retreat(late_q, early)


def group_back_kernel(place, q0, q1, q2, q3, xs, out, qs):
    n = xs.shape[2]
    ordered(place[1], (q0, q1, q2, q3), qs)
    q = qs[3]
    for k in (2, 1, 0):
        q = qs[k] + retreat(q, xs[k, 0:n, :])
    out[...] = q


def smooth_kernel(place, table, gy0, gy1, gy2, gy3, ys, rests, offsets,
                  past, change, his, los,
                  smoothed, high, low, keep, give, gys, values, moment):
    nb = 4
    nseg = 4
    ordered(place[0], (gy0, gy1, gy2, gy3), gys)
    n = gy0.shape[1]
    back = jnp.zeros((8, n), F32)

    def over(k, s):
        j = nseg - 1 - k
        return gys[j] + retreat(s, ys[j, 0:n, :])

    back = lax.fori_loop(0, nseg - 1 - place[0], over, back)
    at = lax.broadcasted_iota(jnp.int32, (BLOCK, n), 0)
    for b in range(nb):
        s = offsets[b] + retreat(back, rests[b])
        step = s - dot3(split(s), (his[b], los[b]))
        values[b] = change[b] + jnp.where(at == BLOCK - 1, step[0:1], 0.0)
    scan_rows(values, his, los, nb, False)
    root_inv = lax.rsqrt(1.0 - decay_of(table, n))
    for b in range(nb):
        smoothed[b * BLOCK : (b + 1) * BLOCK, :] = (values[b] + past[b]) * root_inv
    pair = split(smoothed[...])
    high[...], low[...] = pair
    store_packed(moment, dot3(pair, pair, ((0,), (0,))) * (1.0 / (128 * BLOCK)))
    rows = keep.shape[0]
    keep[...] = moment[pl.ds(pl.multiple_of(place[2] * BLOCK, BLOCK), rows), :]
    give[...] = moment[pl.ds(pl.multiple_of((1 - place[2]) * BLOCK, BLOCK), rows), :]


def errors_kernel(panel_of, table, high, low, observed, turned, sums_out):
    nb = 4
    n = sums_out.shape[1]
    series = turned.shape[1]
    coef = turned[...]
    weight = table[0:4, :]
    squares = jnp.zeros((1, series), F32)
    for b in range(nb):
        part = slice(b * BLOCK, (b + 1) * BLOCK)
        miss = observed[part, :].astype(F32) - (dot(high[part, :], coef) + dot(low[part, :], coef))
        squares = squares + jnp.sum(miss * miss, axis=0, keepdims=True) * weight[b : b + 1]
    counts = float(BLOCK) * jnp.sum(weight, axis=0, keepdims=True)
    lane = lax.broadcasted_iota(jnp.int32, (8, n), 1)
    line = lax.broadcasted_iota(jnp.int32, (8, n), 0)
    sums = jnp.zeros((8, n), F32)
    for j in range(series // SER_BLOCK):
        part = slice(j * SER_BLOCK, (j + 1) * SER_BLOCK)
        sq = jnp.sum(squares[:, part], axis=1, keepdims=True)
        ct = jnp.sum(counts[:, part], axis=1, keepdims=True)
        here = lane == panel_of[j]
        sums = sums + jnp.where(here & (line == 0), sq, 0.0) + jnp.where(here & (line == 1), ct, 0.0)
    sums_out[...] = sums


def moment_kernel(place, table, high, low, observed, own_part, far_part, moment):
    nb = 4
    weight = table[0:4, :]
    kept = jnp.concatenate(
        [
            (observed[b * BLOCK : (b + 1) * BLOCK, :].astype(F32) * weight[b : b + 1]).astype(BF16)
            for b in range(nb)
        ],
        axis=0,
    )
    both = ((0,), (0,))
    scale = 1.0 / math.sqrt(128 * BLOCK)
    moment[...] = (dot(high[...], kept, both) + dot(low[...], kept, both)) * scale
    for i in range(16):
        own = moment[pl.ds(pl.multiple_of((2 * i + place[2]) * 8, 8), 8), :]
        far = moment[pl.ds(pl.multiple_of((2 * i + 1 - place[2]) * 8, 8), 8), :]
        for j in range(8):
            own_part[i, 8 * j : 8 * j + 8, :] = own[:, j * 128 : (j + 1) * 128]
            far_part[i, 8 * j : 8 * j + 8, :] = far[:, j * 128 : (j + 1) * 128]


def add_kernel(a, b, out):
    out[...] = a[...] + b[...]


def small_kernel(keep, given, s, s_far, out):
    n = keep.shape[0]
    out[0:n, :] = keep[...] + given[...]
    out[n:, :] = s[...] + s_far[...]


def collect_kernel(arrived, out):
    total = jnp.sum(arrived[...], axis=0)
    for j in range(8):
        out[:, j * 128 : (j + 1) * 128] = total[8 * j : 8 * j + 8]


def variance_kernel(s0, s1, s2, s3, out):
    sums = (s0[...] + s1[...]) + (s2[...] + s3[...])
    out[...] = sums[0:1] / jnp.maximum(sums[1:2], 1.0)


def last_sum_kernel(a, b, c, d, state, sums):
    n = state.shape[0]
    total = (a[...] + b[...]) + (c[...] + d[...])
    state[...] = total[:n]
    sums[...] = total[n:]


def sum_kernel(a, b, c, d, out):
    out[...] = (a[...] + b[...]) + (c[...] + d[...])


def finish_kernel(place, mine, other, out):
    first = jnp.where(place[2] == 0, mine[...], other[...])
    second = jnp.where(place[2] == 0, other[...], mine[...])
    out[...] = unpack(jnp.concatenate([first[0:BLOCK], second], axis=0))


def call(kernel, outs, scratch, *args, smem=1, mib=12):
    shapes = [jax.ShapeDtypeStruct(s, d) for s, d in outs]
    specs = [SMEM] * smem + [VMEM] * (len(args) - smem)
    made = pl.pallas_call(
        kernel,
        out_shape=shapes,
        in_specs=specs,
        out_specs=[VMEM] * len(outs),
        scratch_shapes=[pltpu.VMEM(s, d) for s, d in scratch],
        compiler_params=pltpu.CompilerParams(vmem_limit_bytes=mib << 20),
    )
    return made(*args)


def from_peers(arrays, axis):
    n = lax.axis_size(axis)
    out = {0: arrays[0]}
    for k in reversed(range(1, n)):
        out[k] = lax.ppermute(arrays[k], axis, [(i, (i + k) % n) for i in range(n)])
    return [out[k] for k in range(n)]


def gather(array, axis):
    return from_peers([array] * lax.axis_size(axis), axis)


def swap(array, axis):
    return lax.ppermute(array, axis, [(0, 1), (1, 0)])


def step(observed, present, loadings, noise_var, decay_rate, panel_of_block):
    time_rows, series = observed.shape
    width = loadings.shape[1]
    nb = time_rows // BLOCK
    half = width // 2
    ay, ax, ac = TM
    iy, ix, ic, iz = (lax.axis_index(a) for a in (ay, ax, ac, "panel"))
    scalar = lambda *v: jnp.stack([jnp.int32(i) for i in v])
    place = scalar(iy, ix, ic, iz)
    packed = ((width + 8, half), F32)
    map_shape = ((width + 8, width), F32)
    half_shape = ((half + 8, width), F32)
    vec = ((8, width), F32)
    vecs4 = ((4, 8, width), F32)
    maps4 = ((4, width + 8, width), F32)
    rows2 = ((BLOCK, width), F32)
    rows3 = ((nb, BLOCK, width), F32)
    square = ((width, width), F32)
    squares4 = ((nb, width, width), F32)
    powers = ((LEVELS * nb, width, width), BF16)

    both = jnp.concatenate([noise_var, decay_rate]).reshape(1, series + width)
    table, loads, *grams = call(
        gram_kernel, [((16, series), F32), (loadings.shape, BF16)] + [packed] * nb, [], place, present, both, loadings
    )
    projs = call(project_kernel, [rows2] * nb, [], place, table, loads, observed)
    grams = from_peers(grams, "panel")
    projs = from_peers(projs, "panel")
    (err,) = call(inverse_kernel, [packed], [square], table, *grams, smem=0)
    errs = gather(err, "panel")
    proj, end = call(end_kernel, [rows2, vec], [square], table, err, *projs, smem=0)
    ends = gather(end, "panel")
    his, los, tops, seg = call(
        powers_kernel, [powers, powers, squares4, square], [squares4], place, *errs
    )
    seg, proj = lax.optimization_barrier((seg, proj))
    seg_far = swap(seg, ac)
    ends, seg_end = call(segment_end_kernel, [vecs4, vec], [], place, tops, *ends)
    end_far = swap(seg_end, ac)
    projs = gather(proj, "panel")
    pair, pair_half = call(pair_kernel, [map_shape, half_shape], [], place, seg, seg_far, seg_end, end_far)
    (turned,) = call(turn_kernel, [((width, series), BF16)], [], loads, smem=0)
    near = gather(pair_half, ax)[1:]
    group, group_half, xs = call(
        group_kernel, [map_shape, half_shape, maps4], [],
        place, pair, *near, *[swap(m, ac) for m in near],
    )
    near = gather(group_half, ay)[1:]
    starts, rests = call(
        prefix_kernel, [maps4, squares4], [], place, xs, seg_far, end_far, tops, ends
    )
    past, change, firsts, first, ys = call(
        forward_kernel,
        [rows3, rows3, vecs4, vec, maps4],
        [rows3, vecs4],
        place, table, group, *near, *[swap(m, ac) for m in near],
        starts, *projs, his, los, tops,
    )
    first_far = swap(first, ac)
    (pair_first,) = call(pair_back_kernel, [vec], [], place, first, first_far, seg, seg_far)
    group_first, gxs = call(group_back_kernel, [vec, vecs4], [], place, *gather(pair_first, ax), xs)
    flat = ((time_rows, width), BF16)
    piece = ((BLOCK + 8, half), F32)
    firsts_y = gather(group_first, ay)
    (offsets,) = call(suffix_kernel, [vecs4], [], place, gxs, xs, first_far, seg_far, tops, firsts)
    smoothed, high, low, keep, give = call(
        smooth_kernel,
        [((time_rows, width), F32), flat, flat, piece, piece],
        [vecs4, rows3, packed],
        place, table, *firsts_y, ys, rests, offsets, past, change, his, los,
    )
    given = swap(give, ac)
    line = ((8, half), F32)
    (sums,) = call(errors_kernel, [line], [], panel_of_block, table, high, low, observed, turned)
    tall = ((BLOCK + 16, half), F32)
    (small,) = call(small_kernel, [tall], [], keep, given, sums, swap(sums, ac), smem=0)
    smalls = gather(small, ax)
    part = ((16, 64, half), F32)
    own_part, far_part = call(
        moment_kernel, [part, part], [((width, series), F32)], place, table, high, low, observed
    )
    (spread,) = call(add_kernel, [part], [], own_part, swap(far_part, ac), smem=0)
    arrived = lax.all_to_all(spread, (ay, ax), 0, 0, tiled=True)
    (small,) = call(sum_kernel, [tall], [], *smalls, smem=0)
    smalls = gather(small, ay)
    state, sums = call(last_sum_kernel, [piece, line], [], *smalls, smem=0)
    (state_moment,) = call(finish_kernel, [square], [], place, state, swap(state, ac))
    (var,) = call(variance_kernel, [((1, half), F32)], [], *gather(sums, "panel"), smem=0)
    (loading_moment,) = call(collect_kernel, [((8, series), F32)], [], arrived, smem=0)
    return smoothed, loading_moment, state_moment, var[0, :PANELS]


def solution(mesh):
    finer = Mesh(
        mesh.devices.reshape(4, 4, 2, mesh.shape["panel"]), ("tm_0", "tm_1", "tm_2", "panel")
    )
    in_specs = (P(TM, "panel"), P(TM, "panel"), P("panel", None), P("panel"), P(), P("panel"))
    out_specs = (P(TM, None), P(TM, "panel"), P(), P())
    return jax.shard_map(step, mesh=finer, in_specs=in_specs, out_specs=out_specs, check_vma=False)
```

```python
import math

import jax
import jax.numpy as jnp
from jax import lax
from jax.experimental import pallas as pl
from jax.experimental.pallas import tpu as pltpu
from jax.sharding import Mesh
from jax.sharding import PartitionSpec as P


SER_BLOCK = 128
PANELS = 19
LEVELS = 7
BLOCK = 128
TM = ("tm_0", "tm_1", "tm_2")
F32 = jnp.float32
BF16 = jnp.bfloat16
HIGH = lax.Precision.HIGHEST
VMEM = pl.BlockSpec(memory_space=pltpu.VMEM)
SMEM = pl.BlockSpec(memory_space=pltpu.SMEM)


def split(x):
    hi = x.astype(BF16)
    return hi, (x - hi.astype(F32)).astype(BF16)


def dot(a, b, dims=((1,), (0,))):
    return lax.dot_general(a, b, (dims, ((), ())), preferred_element_type=F32)


def stacked(parts, b):
    rows = parts[0].shape[0]
    both = dot(jnp.concatenate(parts, axis=0), b)
    return both[:rows] + both[rows:]


def dot3(a, b, dims=((1,), (0,))):
    rows = a[0].shape[0]
    if dims[0] == (1,):
        both = dot(jnp.concatenate(a, axis=0), b[0], dims)
        return (both[:rows] + both[rows:]) + dot(a[0], b[1], dims)
    return dot(a[0], b[0], dims) + (dot(a[0], b[1], dims) + dot(a[1], b[0], dims))


def grid_iota(n, axis):
    return lax.broadcasted_iota(jnp.int32, (n, n), axis)


def eye(n):
    return (grid_iota(n, 0) == grid_iota(n, 1)).astype(F32)


def pack(sym):
    n = sym.shape[0] // 2
    first, corner, second = sym[:n, :n], sym[:n, n:], sym[n:, n:]
    mixed = jnp.where(grid_iota(n, 0) >= grid_iota(n, 1), first, second)
    diag = jnp.sum(second * eye(n), axis=0, keepdims=True)
    return corner, mixed, jnp.broadcast_to(diag, (8, n))


def store_packed(ref, sym):
    n = sym.shape[0] // 2
    corner, mixed, diag = pack(sym)
    ref[0:n, :] = corner
    ref[n : 2 * n, :] = mixed
    ref[2 * n : 2 * n + 8, :] = diag


def unpack(packed):
    n = packed.shape[1]
    corner, mixed, diag = packed[:n], packed[n : 2 * n], packed[2 * n : 2 * n + 1]
    turned = mixed.T
    row, col = grid_iota(n, 0), grid_iota(n, 1)
    first = jnp.where(row >= col, mixed, turned)
    second = jnp.where(row == col, diag, jnp.where(row < col, mixed, turned))
    return jnp.concatenate(
        [jnp.concatenate([first, corner], axis=1), jnp.concatenate([corner.T, second], axis=1)],
        axis=0,
    )


def gram_kernel(place, present, both, loads, table, kept_loads, *outs):
    coef = loads[...]
    kept_loads[...] = coef
    series, n = coef.shape
    mask = present[...].astype(F32)
    inv_noise = 1.0 / both[:, 0:series]
    table[0:4, :] = mask
    table[4:5, 0:n] = both[:, series:]
    table[8:12, :] = mask * inv_noise
    high, low = split(coef.T.astype(F32) * inv_noise)
    for k, out in enumerate(outs):
        kept = table[pl.ds(lax.rem(place[3] + k, len(outs)), 1), :].astype(BF16)
        store_packed(out, stacked((high * kept, low * kept), coef))


def project_kernel(place, table, loads, observed, *outs):
    coef = loads[...]
    for k in range(len(outs)):
        b = lax.rem(place[3] + k, len(outs))
        rows = observed[pl.ds(pl.multiple_of(b * BLOCK, BLOCK), BLOCK), :].astype(F32)
        outs[k][...] = stacked(split(rows * table[pl.ds(8 + b, 1), :]), coef)


def turn_kernel(loads, out):
    out[...] = loads[...].astype(F32).T.astype(BF16)


def decay_of(table, n):
    return table[4:5, 0:n]


def inverse_kernel(table, g0, g1, g2, g3, out, guess):
    gram = unpack((g0[...] + g1[...]) + (g2[...] + g3[...]))
    n = gram.shape[0]
    ident = eye(n)
    whole = ident + gram
    size = jnp.max(jnp.sum(jnp.abs(gram), axis=1, keepdims=True))
    frob = jnp.sqrt(jnp.max(jnp.sum(jnp.sum(gram * gram, axis=1, keepdims=True), axis=0, keepdims=True)))
    top = 1.0 + jnp.minimum(size, frob) * 1.001
    scale = 2.0 / (1.0 + top)
    start = (top - 1.0) / (top + 1.0)
    guess[...] = (2.0 * scale) * ident - (scale * scale) * whole

    def improve(x):
        rest = 2.0 * ident - jnp.dot(whole, x, precision=HIGH, preferred_element_type=F32)
        return jnp.dot(x, rest, precision=HIGH, preferred_element_type=F32)

    def body(err):
        guess[...] = improve(guess[...])
        return err * err

    def quick(err):
        x = guess[...]
        pair = split(x)
        guess[...] = 2.0 * x - dot3(pair, split(dot3(split(whole), pair)))
        return err * err

    err = lax.while_loop(lambda e: (e > 2e-4) & (top < 8.0), quick, start * start)
    lax.while_loop(lambda e: e > 3.9e-8, body, err)
    inverse = guess[...]
    gain = jnp.dot(gram, inverse, precision=HIGH, preferred_element_type=F32)
    gain = 0.5 * (gain + gain.T)
    rho = 1.0 - decay_of(table, n)
    root = jnp.sqrt(rho)
    root_down = jnp.sum(ident * root, axis=1, keepdims=True)
    store_packed(out, ident * (1.0 - rho) + gain * root * root_down)


def shifted(rows, offset, ahead):
    n = rows.shape[0]
    at = lax.broadcasted_iota(jnp.int32, rows.shape, 0)
    if ahead:
        return jnp.where(at >= offset, pltpu.roll(rows, offset, 0), 0.0)
    return jnp.where(at < n - offset, pltpu.roll(rows, n - offset, 0), 0.0)


def end_kernel(table, packed, p0, p1, p2, p3, total, out, err_ref):
    proj = (p0[...] + p1[...]) + (p2[...] + p3[...])
    total[...] = proj
    z = proj * lax.rsqrt(1.0 - decay_of(table, proj.shape[1]))
    err_ref[...] = unpack(packed[...])
    v = z - dot3(split(z), split(err_ref[...]))
    for level in range(LEVELS):
        pair = split(err_ref[...])
        v = v + shifted(v - dot3(split(v), pair), 1 << level, True)
        if level + 1 < LEVELS:
            err_ref[...] = 2.0 * err_ref[...] - dot3(pair, pair)
    out[...] = jnp.broadcast_to(v[BLOCK - 1 :], out.shape)


def powers_kernel(place, e0, e1, e2, e3, his, los, tops, whole, errs):
    nb = 4
    for k, e in enumerate((e0, e1, e2, e3)):
        errs[lax.rem(place[3] + nb - k, nb)] = unpack(e[...])

    def square(level):
        for b in range(nb):
            err = errs[b]
            pair = split(err)
            his[level * nb + b] = pair[0]
            los[level * nb + b] = pair[1]
            errs[b] = 2.0 * err - dot3(pair, pair)

    def squares(k, carry):
        square(2 * k)
        square(2 * k + 1)
        return carry

    lax.fori_loop(0, LEVELS // 2, squares, 0)
    square(LEVELS - 1)
    total = errs[0]
    tops[0] = total
    for b in range(1, nb):
        err = errs[b]
        tops[b] = err
        total = total + err - dot3(split(total), split(err))
    whole[...] = total


def segment_end_kernel(place, tops, v0, v1, v2, v3, ends, out):
    nb = 4
    ordered(place[3], (v0, v1, v2, v3), ends)
    end = ends[0]
    for b in range(1, nb):
        end = end - dot3(split(end), split(tops[b])) + ends[b]
    out[...] = end


def join(maps):
    n = maps[0].shape[1]
    total, end = maps[0][:n], maps[0][n:]
    for m in maps[1:]:
        err = m[:n]
        pair = split(err)
        end = end - dot3(split(end), pair) + m[n:]
        total = total + err - dot3(split(total), pair)
    return total, end


def store_map(total, end, core, out, half):
    n = total.shape[1]
    h = n // 2
    out[0:n, :] = total
    out[n:, :] = end
    half[0:h, :] = out[pl.ds(pl.multiple_of(core * h, h), h), :]
    half[h:, :] = end


def pair_kernel(place, mine, other, v_mine, v_other, out, half):
    own, far, v_own, v_far = mine[...], other[...], v_mine[...], v_other[...]
    first = place[2] == 0
    total = jnp.where(first, own, far)
    err = jnp.where(first, far, own)
    pair = split(err)
    end = jnp.where(first, v_own, v_far)
    end = end - dot3(split(end), pair) + jnp.where(first, v_far, v_own)
    total = total + err - dot3(split(total), pair)
    store_map(total, end, place[2], out, half)


def ordered(place, refs, scratch):
    for k, r in enumerate(refs):
        scratch[lax.rem(place + len(refs) - k, len(refs))] = r[...]


def ordered_maps(place, core, own, halves, maps):
    n = own.shape[1]
    h = n // 2
    maps[place] = own[...]
    for k, (mine, other) in enumerate(halves):
        at = lax.rem(place + 3 - k, 4)
        maps[at, pl.ds(pl.multiple_of(core * h, h), h), :] = mine[0:h, :]
        maps[at, pl.ds(pl.multiple_of((1 - core) * h, h), h), :] = other[0:h, :]
        maps[at, n:, :] = mine[h:, :]


def group_kernel(place, own, m1, m2, m3, o1, o2, o3, out, half, maps):
    ordered_maps(place[1], place[2], own, ((m1, o1), (m2, o2), (m3, o3)), maps)
    total, end = join([maps[k] for k in range(4)])
    store_map(total, end, place[2], out, half)


def advance(state, m):
    n = state.shape[1]
    return state - dot3(split(state), split(m[:n])) + m[n:]


def retreat(state, err):
    return state - dot3(split(state), split(err), ((1,), (1,)))


def scan_rows(values, his, los, nb, ahead):
    for level in range(LEVELS):
        for b in range(nb):
            v = values[b]
            pair = (his[level * nb + b], los[level * nb + b])
            values[b] = v + shifted(v - dot3(split(v), pair), 1 << level, ahead)


def prefix_kernel(place, xs, other, v_other, tops, ends, starts, rests):
    nb = 4
    n = other.shape[1]

    def after(total, end, err, v):
        pair = split(err)
        return total + err - dot3(split(total), pair), end - dot3(split(end), pair) + v

    starts[0] = jnp.zeros((n + 8, n), F32)

    def into(k, carry):
        starts[0, 0:n, :], starts[0, n:, :] = after(
            starts[0, 0:n, :], starts[0, n:, :], xs[k, 0:n, :], xs[k, n:, :]
        )
        return carry

    lax.fori_loop(0, place[1], into, 0)

    @pl.when(place[2] == 1)
    def _():
        starts[0, 0:n, :], starts[0, n:, :] = after(
            starts[0, 0:n, :], starts[0, n:, :], other[...], v_other[...]
        )

    def before(err, total):
        return total + err - dot3(split(err), split(total))

    rests[nb - 1] = jnp.zeros((n, n), F32)

    def back(k, carry):
        rests[nb - 1] = before(xs[3 - k, 0:n, :], rests[nb - 1])
        return carry

    lax.fori_loop(0, 3 - place[1], back, 0)

    @pl.when(place[2] == 0)
    def _():
        rests[nb - 1] = before(other[...], rests[nb - 1])

    def blocks(b, carry):
        starts[b + 1, 0:n, :], starts[b + 1, n:, :] = after(
            starts[b, 0:n, :], starts[b, n:, :], tops[b], ends[b]
        )
        late = nb - 1 - b
        rests[late - 1] = before(tops[late], rests[late])
        return carry

    lax.fori_loop(0, nb - 1, blocks, 0)


def suffix_kernel(place, qs, xs, far, other, tops, firsts, offsets):
    nb = 4
    n = other.shape[1]

    def over(k, s):
        j = 3 - k
        return qs[j] + retreat(s, xs[j, 0:n, :])

    back = lax.fori_loop(0, 3 - place[1], over, jnp.zeros((8, n), F32))
    back = jnp.where(place[2] == 0, far[...] + retreat(back, other[...]), back)
    for b in reversed(range(nb)):
        offsets[b] = back
        if b:
            back = back - dot3(split(back), split(tops[b])) + firsts[b]


def forward_kernel(place, table, own, m1, m2, m3, o1, o2, o3, starts, p0, p1, p2, p3,
                   his, los, tops,
                   past, change, firsts, first, ys, values, states):
    nb = 4
    n = own.shape[1]
    rho = 1.0 - decay_of(table, n)
    root_inv = lax.rsqrt(rho)
    ordered(place[3], (p0, p1, p2, p3), values)
    ordered_maps(place[0], place[2], own, ((m1, o1), (m2, o2), (m3, o3)), ys)
    state = jnp.zeros((8, n), F32)
    state = lax.fori_loop(0, place[0], lambda k, s: advance(s, ys[k]), state)
    at = lax.broadcasted_iota(jnp.int32, (BLOCK, n), 0)
    for b in range(nb):
        states[b] = advance(state, starts[b])
    for b in range(nb):
        z = values[b] * root_inv
        z = z + jnp.where(at == 0, states[b][0:1], 0.0)
        values[b] = z - dot3(split(z), (his[b], los[b]))
    scan_rows(values, his, los, nb, True)
    for b in range(nb):
        v = values[b]
        before = jnp.where(at == 0, states[b][0:1], pltpu.roll(v, 1, 0)) * rho
        past[b] = before
        change[b] = v - before
        values[b] = v - before
    scan_rows(values, his, los, nb, False)
    back = jnp.zeros((8, n), F32)
    for b in reversed(range(nb)):
        lead = jnp.broadcast_to(values[b][0:1], (8, n))
        firsts[b] = lead
        back = back - dot3(split(back), split(tops[b])) + lead
    first[...] = back


def pair_back_kernel(place, own, far, mine, other, out):
    lead = place[2] == 0
    early_q = jnp.where(lead, own[...], far[...])
    late_q = jnp.where(lead, far[...], own[...])
    early = jnp.where(lead, mine[...], other[...])
    out[...] = early_q + retreat(late_q, early)


def group_back_kernel(place, q0, q1, q2, q3, xs, out, qs):
    n = xs.shape[2]
    ordered(place[1], (q0, q1, q2, q3), qs)
    q = qs[3]
    for k in (2, 1, 0):
        q = qs[k] + retreat(q, xs[k, 0:n, :])
    out[...] = q


def smooth_kernel(place, table, gy0, gy1, gy2, gy3, ys, rests, offsets,
                  past, change, his, los,
                  smoothed, high, low, keep, give, gys, values, moment):
    nb = 4
    nseg = 4
    ordered(place[0], (gy0, gy1, gy2, gy3), gys)
    n = gy0.shape[1]
    back = jnp.zeros((8, n), F32)

    def over(k, s):
        j = nseg - 1 - k
        return gys[j] + retreat(s, ys[j, 0:n, :])

    back = lax.fori_loop(0, nseg - 1 - place[0], over, back)
    at = lax.broadcasted_iota(jnp.int32, (BLOCK, n), 0)
    for b in range(nb):
        s = offsets[b] + retreat(back, rests[b])
        step = s - dot3(split(s), (his[b], los[b]))
        values[b] = change[b] + jnp.where(at == BLOCK - 1, step[0:1], 0.0)
    scan_rows(values, his, los, nb, False)
    root_inv = lax.rsqrt(1.0 - decay_of(table, n))
    for b in range(nb):
        smoothed[b * BLOCK : (b + 1) * BLOCK, :] = (values[b] + past[b]) * root_inv
    pair = split(smoothed[...])
    high[...], low[...] = pair
    store_packed(moment, dot3(pair, pair, ((0,), (0,))) * (1.0 / (128 * BLOCK)))
    rows = keep.shape[0]
    keep[...] = moment[pl.ds(pl.multiple_of(place[2] * BLOCK, BLOCK), rows), :]
    give[...] = moment[pl.ds(pl.multiple_of((1 - place[2]) * BLOCK, BLOCK), rows), :]


def errors_kernel(panel_of, table, high, low, observed, turned, sums_out):
    nb = 4
    n = sums_out.shape[1]
    series = turned.shape[1]
    coef = turned[...]
    weight = table[0:4, :]
    squares = jnp.zeros((1, series), F32)
    for b in range(nb):
        part = slice(b * BLOCK, (b + 1) * BLOCK)
        miss = observed[part, :].astype(F32) - stacked((high[part, :], low[part, :]), coef)
        squares = squares + jnp.sum(miss * miss, axis=0, keepdims=True) * weight[b : b + 1]
    counts = float(BLOCK) * jnp.sum(weight, axis=0, keepdims=True)
    lane = lax.broadcasted_iota(jnp.int32, (8, n), 1)
    line = lax.broadcasted_iota(jnp.int32, (8, n), 0)
    sums = jnp.zeros((8, n), F32)
    for j in range(series // SER_BLOCK):
        part = slice(j * SER_BLOCK, (j + 1) * SER_BLOCK)
        sq = jnp.sum(squares[:, part], axis=1, keepdims=True)
        ct = jnp.sum(counts[:, part], axis=1, keepdims=True)
        here = lane == panel_of[j]
        sums = sums + jnp.where(here & (line == 0), sq, 0.0) + jnp.where(here & (line == 1), ct, 0.0)
    sums_out[...] = sums


def moment_kernel(place, table, high, low, observed, own_part, far_part, moment):
    nb = 4
    weight = table[0:4, :]
    kept = jnp.concatenate(
        [
            (observed[b * BLOCK : (b + 1) * BLOCK, :].astype(F32) * weight[b : b + 1]).astype(BF16)
            for b in range(nb)
        ],
        axis=0,
    )
    both = ((0,), (0,))
    scale = 1.0 / math.sqrt(128 * BLOCK)
    moment[...] = (dot(high[...], kept, both) + dot(low[...], kept, both)) * scale
    for i in range(16):
        own = moment[pl.ds(pl.multiple_of((2 * i + place[2]) * 8, 8), 8), :]
        far = moment[pl.ds(pl.multiple_of((2 * i + 1 - place[2]) * 8, 8), 8), :]
        for j in range(8):
            own_part[i, 8 * j : 8 * j + 8, :] = own[:, j * 128 : (j + 1) * 128]
            far_part[i, 8 * j : 8 * j + 8, :] = far[:, j * 128 : (j + 1) * 128]


def add_kernel(a, b, out):
    out[...] = a[...] + b[...]


def small_kernel(keep, given, s, s_far, out):
    n = keep.shape[0]
    out[0:n, :] = keep[...] + given[...]
    out[n:, :] = s[...] + s_far[...]


def collect_kernel(arrived, out):
    total = jnp.sum(arrived[...], axis=0)
    for j in range(8):
        out[:, j * 128 : (j + 1) * 128] = total[8 * j : 8 * j + 8]


def variance_kernel(s0, s1, s2, s3, out):
    sums = (s0[...] + s1[...]) + (s2[...] + s3[...])
    out[...] = sums[0:1] / jnp.maximum(sums[1:2], 1.0)


def last_sum_kernel(a, b, c, d, state, sums):
    n = state.shape[0]
    total = (a[...] + b[...]) + (c[...] + d[...])
    state[...] = total[:n]
    sums[...] = total[n:]


def sum_kernel(a, b, c, d, out):
    out[...] = (a[...] + b[...]) + (c[...] + d[...])


def finish_kernel(place, mine, other, out):
    first = jnp.where(place[2] == 0, mine[...], other[...])
    second = jnp.where(place[2] == 0, other[...], mine[...])
    out[...] = unpack(jnp.concatenate([first[0:BLOCK], second], axis=0))


def call(kernel, outs, scratch, *args, smem=1, mib=12):
    shapes = [jax.ShapeDtypeStruct(s, d) for s, d in outs]
    specs = [SMEM] * smem + [VMEM] * (len(args) - smem)
    made = pl.pallas_call(
        kernel,
        out_shape=shapes,
        in_specs=specs,
        out_specs=[VMEM] * len(outs),
        scratch_shapes=[pltpu.VMEM(s, d) for s, d in scratch],
        compiler_params=pltpu.CompilerParams(vmem_limit_bytes=mib << 20),
    )
    return made(*args)


def from_peers(arrays, axis):
    n = lax.axis_size(axis)
    out = {0: arrays[0]}
    for k in reversed(range(1, n)):
        out[k] = lax.ppermute(arrays[k], axis, [(i, (i + k) % n) for i in range(n)])
    return [out[k] for k in range(n)]


def gather(array, axis):
    return from_peers([array] * lax.axis_size(axis), axis)


def swap(array, axis):
    return lax.ppermute(array, axis, [(0, 1), (1, 0)])


def step(observed, present, loadings, noise_var, decay_rate, panel_of_block):
    time_rows, series = observed.shape
    width = loadings.shape[1]
    nb = time_rows // BLOCK
    half = width // 2
    ay, ax, ac = TM
    iy, ix, ic, iz = (lax.axis_index(a) for a in (ay, ax, ac, "panel"))
    scalar = lambda *v: jnp.stack([jnp.int32(i) for i in v])
    place = scalar(iy, ix, ic, iz)
    packed = ((width + 8, half), F32)
    map_shape = ((width + 8, width), F32)
    half_shape = ((half + 8, width), F32)
    vec = ((8, width), F32)
    vecs4 = ((4, 8, width), F32)
    maps4 = ((4, width + 8, width), F32)
    rows2 = ((BLOCK, width), F32)
    rows3 = ((nb, BLOCK, width), F32)
    square = ((width, width), F32)
    squares4 = ((nb, width, width), F32)
    powers = ((LEVELS * nb, width, width), BF16)

    both = jnp.concatenate([noise_var, decay_rate]).reshape(1, series + width)
    table, loads, *grams = call(
        gram_kernel, [((16, series), F32), (loadings.shape, BF16)] + [packed] * nb, [], place, present, both, loadings
    )
    projs = call(project_kernel, [rows2] * nb, [], place, table, loads, observed)
    grams = from_peers(grams, "panel")
    projs = from_peers(projs, "panel")
    (err,) = call(inverse_kernel, [packed], [square], table, *grams, smem=0)
    errs = gather(err, "panel")
    proj, end = call(end_kernel, [rows2, vec], [square], table, err, *projs, smem=0)
    ends = gather(end, "panel")
    his, los, tops, seg = call(
        powers_kernel, [powers, powers, squares4, square], [squares4], place, *errs
    )
    seg, proj = lax.optimization_barrier((seg, proj))
    seg_far = swap(seg, ac)
    ends, seg_end = call(segment_end_kernel, [vecs4, vec], [], place, tops, *ends)
    end_far = swap(seg_end, ac)
    projs = gather(proj, "panel")
    pair, pair_half = call(pair_kernel, [map_shape, half_shape], [], place, seg, seg_far, seg_end, end_far)
    (turned,) = call(turn_kernel, [((width, series), BF16)], [], loads, smem=0)
    near = gather(pair_half, ax)[1:]
    group, group_half, xs = call(
        group_kernel, [map_shape, half_shape, maps4], [],
        place, pair, *near, *[swap(m, ac) for m in near],
    )
    near = gather(group_half, ay)[1:]
    starts, rests = call(
        prefix_kernel, [maps4, squares4], [], place, xs, seg_far, end_far, tops, ends
    )
    past, change, firsts, first, ys = call(
        forward_kernel,
        [rows3, rows3, vecs4, vec, maps4],
        [rows3, vecs4],
        place, table, group, *near, *[swap(m, ac) for m in near],
        starts, *projs, his, los, tops,
    )
    first_far = swap(first, ac)
    (pair_first,) = call(pair_back_kernel, [vec], [], place, first, first_far, seg, seg_far)
    group_first, gxs = call(group_back_kernel, [vec, vecs4], [], place, *gather(pair_first, ax), xs)
    flat = ((time_rows, width), BF16)
    piece = ((BLOCK + 8, half), F32)
    firsts_y = gather(group_first, ay)
    (offsets,) = call(suffix_kernel, [vecs4], [], place, gxs, xs, first_far, seg_far, tops, firsts)
    smoothed, high, low, keep, give = call(
        smooth_kernel,
        [((time_rows, width), F32), flat, flat, piece, piece],
        [vecs4, rows3, packed],
        place, table, *firsts_y, ys, rests, offsets, past, change, his, los,
    )
    given = swap(give, ac)
    line = ((8, half), F32)
    (sums,) = call(errors_kernel, [line], [], panel_of_block, table, high, low, observed, turned)
    tall = ((BLOCK + 16, half), F32)
    (small,) = call(small_kernel, [tall], [], keep, given, sums, swap(sums, ac), smem=0)
    smalls = gather(small, ax)
    part = ((16, 64, half), F32)
    own_part, far_part = call(
        moment_kernel, [part, part], [((width, series), F32)], place, table, high, low, observed
    )
    (spread,) = call(add_kernel, [part], [], own_part, swap(far_part, ac), smem=0)
    arrived = lax.all_to_all(spread, (ay, ax), 0, 0, tiled=True)
    (small,) = call(sum_kernel, [tall], [], *smalls, smem=0)
    smalls = gather(small, ay)
    state, sums = call(last_sum_kernel, [piece, line], [], *smalls, smem=0)
    (state_moment,) = call(finish_kernel, [square], [], place, state, swap(state, ac))
    (var,) = call(variance_kernel, [((1, half), F32)], [], *gather(sums, "panel"), smem=0)
    (loading_moment,) = call(collect_kernel, [((8, series), F32)], [], arrived, smem=0)
    return smoothed, loading_moment, state_moment, var[0, :PANELS]


def solution(mesh):
    finer = Mesh(
        mesh.devices.reshape(4, 4, 2, mesh.shape["panel"]), ("tm_0", "tm_1", "tm_2", "panel")
    )
    in_specs = (P(TM, "panel"), P(TM, "panel"), P("panel", None), P("panel"), P(), P("panel"))
    out_specs = (P(TM, None), P(TM, "panel"), P(), P())
    return jax.shard_map(step, mesh=finer, in_specs=in_specs, out_specs=out_specs, check_vma=False)
```
